32 devices in a mesh: dp: 2 (over core), zero: 16 (over z, y, x).
Axes of the slice: x: 2, y: 2, z: 4, core: 2. Of those that a mesh axis runs over, the one named last changes fastest.
Arguments:
- tokens: bfloat16 [32768, 768], P(('dp', 'zero')), may hold values from -6 to 6
- out_grad: bfloat16 [32768, 768], P(('dp', 'zero')), may hold values from -6 to 6
- mask_pos: int32 [256, 32], P(('dp', 'zero')), may hold values from -1 to 127, as said below
- repl_id: int32 [256, 32], P(('dp', 'zero')), may hold values from 0 to 4095
- replace_embed: bfloat16 [4096, 768], replicated, may hold values from -6 to 6
- masters: float32 [16, 768, 768], P(None, 'zero'), as said below
- norm_params: float32 [4, 768], P(None, 'zero'), as said below
- first_moment: float32 [16, 768, 768], P(None, 'zero')
- second_moment: float32 [16, 768, 768], P(None, 'zero'), as said below
- left_basis: float32 [16, 768, 768], P(None, 'zero'), as said below
- right_basis: float32 [16, 768, 768], P(None, 'zero'), as said below
- norm_first: float32 [4, 768], P(None, 'zero')
- norm_second: float32 [4, 768], P(None, 'zero'), as said below
- step: int32 [1], replicated, may hold values from 1 to 20
Outputs:
- layer_out: bfloat16 [32768, 768], P(('dp', 'zero'))
- in_grad: float32 [32768, 768], P(('dp', 'zero'))
- new_first: float32 [16, 768, 768], P(None, 'zero')
- new_second: float32 [16, 768, 768], P(None, 'zero')
- new_master: float32 [16, 768, 768], P(None, 'zero')
- new_copy: bfloat16 [16, 768, 768], P(None, 'zero')
- new_norm_first: float32 [4, 768], P(None, 'zero')
- new_norm_second: float32 [4, 768], P(None, 'zero')
- new_norms: float32 [4, 768], P(None, 'zero')
The draws below stay inside these ranges and needn't reach their ends.
Inputs may be any that keep to these rules, and one draw needn't show every extreme that they name: `mask_pos`: in each sequence the entries other than -1 are distinct positions and stand in the first slots; a sequence has 1 to 32 of them. `masters`: tiles 0 to 2, the gate and up tiles, tile 3 and the down tiles have entries of deviation about 768^-0.5, (4/768)^0.5, and (2/3072)^0.5. `norm_params`: rows 0 and 2 are gains within 0.7 to 1.3; rows 1 and 3 are shifts. `second_moment`: every entry is positive. `left_basis`: each tile's basis is orthogonal. `right_basis`: each tile's basis is orthogonal. `norm_second`: every entry is positive.
All inputs are finite; a program needn't handle non-finite values.
Results may differ from the reference program's by a relative error of at most 0.0075.
The reference program's roundings to bfloat16 on the way count: a program that leaves them out, or rounds other values in their place, can miss the bound.
Values may be sent and summed in bfloat16 or wider, within the bound.
A program may use at most 256 MiB of HBM per device.

```python
import math
import jax
import jax.numpy as jnp
import numpy as np
from jax import lax

D = 768
HEADS = 12
FF = 3072
VOCAB = 4096
LEN = 128
MASKS = 32
TILES = 16
SEQS = 256
TOKENS = 32768


def unit_noise(noise_key, noise_shape):
    return jnp.clip(jax.random.normal(noise_key, noise_shape, jnp.float32), -4.0, 4.0)


def weight_levels():
    tile_index = jnp.arange(TILES)
    ff_parts = FF // D
    inner_level = float(D) ** (-0.5)
    out_level = float(D // 4) ** (-0.5)
    down_level = float(FF // 2) ** (-0.5)
    return jnp.where(tile_index < 3, inner_level, jnp.where(tile_index == 3, out_level, jnp.where(tile_index < 4 + 2 * ff_parts, inner_level, down_level)))


def grad_levels():
    tile_index = jnp.arange(TILES)
    ff_parts = FF // D
    head_levels = jnp.array([0.5, 0.5, 1.2, 0.25], jnp.float32)
    head_part = jnp.take(head_levels, jnp.minimum(tile_index, 3))
    ff_level = jnp.where(tile_index < 4 + 2 * ff_parts, 0.2, 0.4)
    return jnp.where(tile_index < 4, head_part, ff_level) * math.sqrt(TOKENS)


def spread_factor(factor_key, factor_shape):
    return jnp.exp(jax.random.uniform(factor_key, factor_shape, jnp.float32, 0.0, math.log(4.0)))


def draw_masters(key, part):
    levels = weight_levels()
    return levels[:, None, None] * unit_noise(jax.random.fold_in(key, 1), (TILES, D, D))


def draw_norm_params(key, part):
    gain_key, shift_key = jax.random.split(jax.random.fold_in(key, 2))
    gain_rows = 1.0 + jax.random.uniform(gain_key, (4, D), jnp.float32, -0.3, 0.3)
    shift_rows = 0.3 * unit_noise(shift_key, (4, D))
    row_index = jnp.arange(4)[:, None]
    return jnp.where(row_index % 2 == 0, gain_rows, shift_rows)


def draw_first_moment(key, part):
    levels = grad_levels()
    return 0.1 / 0.9 * levels[:, None, None] * unit_noise(jax.random.fold_in(key, 3), (TILES, D, D))


def draw_second_moment(key, part):
    levels = grad_levels()
    return 0.05 / 0.95 * (levels * levels)[:, None, None] * spread_factor(jax.random.fold_in(key, 4), (TILES, D, D))


def draw_norm_first(key, part):
    level = 0.8 * math.sqrt(TOKENS)
    return 0.1 / 0.9 * level * unit_noise(jax.random.fold_in(key, 5), (4, D))


def draw_norm_second(key, part):
    level = 0.8 * math.sqrt(TOKENS)
    return 0.05 / 0.95 * level * level * spread_factor(jax.random.fold_in(key, 6), (4, D))


def orthogonal_stack(basis_key):
    noise = jax.random.normal(basis_key, (TILES, D, D), jnp.float32)
    basis, upper = jnp.linalg.qr(noise)
    return basis


def draw_left_basis(key, part):
    return orthogonal_stack(jax.random.fold_in(key, 11))


def draw_right_basis(key, part):
    return orthogonal_stack(jax.random.fold_in(key, 13))


def draw_mask_pos(key, part):
    order_key, count_key = jax.random.split(jax.random.fold_in(key, 8))
    row_keys = jax.random.split(order_key, SEQS)

    def row_order(row_key):
        return jax.random.permutation(row_key, LEN)
    orders = jax.vmap(row_order)(row_keys)[:, :MASKS]
    counts = jax.random.randint(count_key, (SEQS, 1), 1, MASKS + 1)
    slot_index = jnp.arange(MASKS)[None, :]
    return jnp.where(slot_index < counts, orders, -1).astype(jnp.int32)


def touch_ends(drawn, key, least, top_value):
    index_at = [jax.random.randint(jax.random.fold_in(key, axis), (), 0, length) for axis, length in enumerate(drawn.shape)]
    main_axis = drawn.shape.index(max(drawn.shape))
    neighbour = index_at[:main_axis] + [(index_at[main_axis] + 1) % drawn.shape[main_axis]] + index_at[main_axis + 1:]
    return drawn.at[tuple(index_at)].set(least).at[tuple(neighbour)].set(top_value)


def block_scale(stream_key, shape, shards, least, top_value):
    loudness, own = 1.0, jax.random.fold_in(stream_key, 6)
    for axis_at, parts in shards:
        heights = jnp.exp(jax.random.uniform(jax.random.fold_in(own, axis_at), (parts,), jnp.float32, least / len(shards), top_value / len(shards)))
        loudness = loudness * jnp.repeat(heights, shape[axis_at] // parts).reshape([-1 if axis == axis_at else 1 for axis in range(len(shape))])
    return loudness


def gaussian(own_key, dims, width, limit, shards=(), kind=jnp.bfloat16):
    factor_of = block_scale(own_key, dims, shards, -0.22, 0.18) if shards else 1.0
    drawn = jax.random.normal(own_key, dims, jnp.float32) * width * factor_of
    return jnp.minimum(jnp.maximum(drawn, -limit), limit).astype(kind)


def setup_inputs(seed: int = 0) -> dict:
    keys = jax.random.split(jax.random.key(seed), 15)
    tokens = gaussian(keys[0], (TOKENS, D), 1.0, 6.0, ((0, 32),))
    out_grad = gaussian(keys[1], (TOKENS, D), 1.0, 6.0, ((0, 32),))
    mask_pos = draw_mask_pos(jax.random.fold_in(keys[14], 71), 0)
    repl_id = touch_ends(jax.random.randint(keys[3], (SEQS, MASKS), 0, VOCAB), jax.random.fold_in(keys[3], 1), 0, VOCAB - 1).astype(jnp.int32)
    replace_embed = gaussian(keys[4], (VOCAB, D), 1.0, 6.0)
    masters = draw_masters(jax.random.fold_in(keys[14], 71), 0)
    norm_params = draw_norm_params(jax.random.fold_in(keys[14], 71), 0)
    first_moment = draw_first_moment(jax.random.fold_in(keys[14], 71), 0)
    second_moment = draw_second_moment(jax.random.fold_in(keys[14], 71), 0)
    left_basis = draw_left_basis(jax.random.fold_in(keys[14], 71), 0)
    right_basis = draw_right_basis(jax.random.fold_in(keys[14], 71), 0)
    norm_first = draw_norm_first(jax.random.fold_in(keys[14], 71), 0)
    norm_second = draw_norm_second(jax.random.fold_in(keys[14], 71), 0)
    step = jax.random.randint(keys[13], (1,), 1, 21).astype(jnp.int32)
    return {"tokens": tokens, "out_grad": out_grad, "mask_pos": mask_pos, "repl_id": repl_id, "replace_embed": replace_embed, "masters": masters, "norm_params": norm_params, "first_moment": first_moment, "second_moment": second_moment, "left_basis": left_basis, "right_basis": right_basis, "norm_first": norm_first, "norm_second": norm_second, "step": step}


@jax.custom_vjp
def low(v):
    return lax.optimization_barrier(v.astype(jnp.bfloat16)).astype(jnp.float32)

@jax.custom_vjp
def low_back(v):
    return v

def low_keep(v):
    return (low(v), None)

def low_pass(kept, grad):
    return (grad,)

def back_keep(v):
    return (v, None)

def back_low(kept, grad):
    return (low(grad),)
low.defvjp(low_keep, low_pass)
low_back.defvjp(back_keep, back_low)
highest = lax.Precision.HIGHEST
norm_eps = 1e-12
beta_one = 0.9
beta_two = 0.95
adam_eps = 1e-08
peak_rate = 0.1
warm_steps = 5.0
total_steps = 60.0
decay_rate = 0.01

def alibi_slopes(head_count):

    def power_slopes(power_count):
        first_slope = 2.0 ** (-8.0 / power_count)
        return [first_slope ** (position + 1) for position in range(power_count)]
    nearest = 2 ** int(math.floor(math.log2(head_count)))
    slope_list = power_slopes(nearest)
    if nearest < head_count:
        slope_list = slope_list + power_slopes(2 * nearest)[0::2][:head_count - nearest]
    return np.array(slope_list, np.float32)

def layer_norm(values, gain_row, shift_row):
    row_mean = lax.optimization_barrier(jnp.mean(values, axis=-1, keepdims=True))
    centered = values - row_mean
    spread = lax.optimization_barrier(jnp.mean(centered * centered, axis=-1, keepdims=True))
    return centered * lax.rsqrt(spread + norm_eps) * gain_row + shift_row

def split_tiles(tile_stack):
    model_width = tile_stack.shape[1]
    ff_parts = (tile_stack.shape[0] - 4) // 3
    gate_w = tile_stack[4:4 + ff_parts].transpose(1, 0, 2).reshape(model_width, ff_parts * model_width)
    up_w = tile_stack[4 + ff_parts:4 + 2 * ff_parts].transpose(1, 0, 2).reshape(model_width, ff_parts * model_width)
    down_w = tile_stack[4 + 2 * ff_parts:].reshape(ff_parts * model_width, model_width)
    return (tile_stack[0], tile_stack[1], tile_stack[2], tile_stack[3], gate_w, up_w, down_w)

def block_forward(inputs, tile_stack, norm_stack, length):
    weights = low(tile_stack)
    norm_gains = low(norm_stack)
    query_w, key_w, value_w, out_w, gate_w, up_w, down_w = split_tiles(weights)
    tok_rows, model_width = inputs.shape
    head_count = HEADS
    head_size = model_width // head_count
    score_scale = float(head_size) ** (-0.5)
    slopes = jnp.asarray(alibi_slopes(head_count))
    positions = jnp.arange(length)
    distance = jnp.abs(positions[:, None] - positions[None, :]).astype(jnp.float32)
    alibi_bias = -slopes[:, None, None] * distance[None]

    def project(weight_tile):
        result = low_back(low(jnp.dot(inputs, weight_tile, precision=highest)))
        return result.reshape(tok_rows // length, length, head_count, head_size)
    queries = project(query_w)
    key_rows = project(key_w)
    values = project(value_w)
    scores = jnp.einsum('bqhd,bkhd->bhqk', queries, key_rows, precision=highest) * score_scale + alibi_bias[None]
    scores = low_back(scores)
    soft_low = low(jax.nn.softmax(scores, axis=-1))
    mixed_low = jnp.einsum('bhqk,bkhd->bqhd', soft_low, values, precision=highest).reshape(tok_rows, model_width)
    mixed_low = low_back(low(mixed_low))
    attended = low_back(jnp.dot(mixed_low, out_w, precision=highest))
    hidden = layer_norm(inputs + attended, norm_gains[0], norm_gains[1])
    hidden_low = low(hidden)
    gate_val = low_back(jnp.dot(hidden_low, gate_w, precision=highest))
    up_value = low_back(jnp.dot(hidden_low, up_w, precision=highest))
    inner_act = low(jax.nn.gelu(gate_val, approximate=False) * up_value)
    branch = low_back(jnp.dot(inner_act, down_w, precision=highest))
    return layer_norm(hidden + branch, norm_gains[2], norm_gains[3])

def reference(tokens, out_grad, mask_pos, repl_id, replace_embed, masters, norm_params, first_moment, second_moment, left_basis, right_basis, norm_first, norm_second, step):
    seq_count = mask_pos.shape[0]
    length = tokens.shape[0] // seq_count
    model_width = tokens.shape[1]
    positions = jnp.arange(length, dtype=jnp.int32)
    mask_hits = mask_pos[:, :, None] == positions[None, None, :]
    masked = jnp.any(mask_hits, axis=1).reshape(-1, 1)
    row_ids = lax.optimization_barrier(jnp.sum(jnp.where(mask_hits, repl_id[:, :, None], 0), axis=1)).reshape(-1).astype(jnp.int32)
    embedded = jnp.take(replace_embed, row_ids, axis=0)
    inputs = jnp.where(masked, embedded, tokens).astype(jnp.float32)
    group_seqs = math.gcd(seq_count, max(1, 4096 // length))
    group_count = seq_count // group_seqs
    stacked_in = inputs.reshape(group_count, group_seqs * length, model_width)
    stacked_cot = out_grad.astype(jnp.float32).reshape(group_count, group_seqs * length, model_width)

    def one_group(carry, pair):
        block_in, block_cot = pair

        def forward_fn(first_arg, second_arg, third_arg):
            return block_forward(first_arg, second_arg, third_arg, length)
        result, pullback = jax.vjp(forward_fn, block_in, masters, norm_params)
        grad_in, grad_tiles, grad_norms = pullback(block_cot)
        return ((carry[0] + grad_tiles, carry[1] + grad_norms), (result, grad_in))
    start = (jnp.zeros_like(masters), jnp.zeros_like(norm_params))
    (tile_grads, norm_grads), (results, grads_in) = lax.scan(one_group, start, (stacked_in, stacked_cot))
    layer_out = results.reshape(-1, model_width).astype(jnp.bfloat16)
    in_grad = jnp.where(masked, 0.0, grads_in.reshape(-1, model_width))
    step_value = step[0].astype(jnp.float32)
    step_rate = peak_rate * jnp.minimum(step_value / warm_steps, (total_steps - step_value) / (total_steps - warm_steps))
    fix_one = 1.0 - jnp.power(beta_one, step_value)
    fix_two = 1.0 - jnp.power(beta_two, step_value)
    rotated = jnp.einsum('tji,tjl->til', left_basis, tile_grads, precision=highest)
    rotated = jnp.einsum('til,tlm->tim', rotated, right_basis, precision=highest)
    new_first = beta_one * first_moment + (1.0 - beta_one) * rotated
    new_second = beta_two * second_moment + (1.0 - beta_two) * rotated * rotated
    direction = new_first / fix_one / (jnp.sqrt(new_second / fix_two) + adam_eps)
    update = jnp.einsum('tij,tjl->til', left_basis, direction, precision=highest)
    update = jnp.einsum('til,tml->tim', update, right_basis, precision=highest)
    new_master = masters - step_rate * (update + decay_rate * masters)
    new_copy = new_master.astype(jnp.bfloat16)
    new_norm_first = beta_one * norm_first + (1.0 - beta_one) * norm_grads
    new_norm_second = beta_two * norm_second + (1.0 - beta_two) * norm_grads * norm_grads
    new_norms = norm_params - step_rate * (new_norm_first / fix_one) / (jnp.sqrt(new_norm_second / fix_two) + adam_eps)
    return (layer_out, in_grad, new_first, new_second, new_master, new_copy, new_norm_first, new_norm_second, new_norms)
```

```python
import math

import jax
import jax.numpy as jnp
import numpy as np
from jax import lax
from jax.sharding import PartitionSpec as P

HEADS = 12

norm_eps = 1e-12
beta_one = 0.9
beta_two = 0.95
adam_eps = 1e-08
peak_rate = 0.1
warm_steps = 5.0
total_steps = 60.0
decay_rate = 0.01
low_type = jnp.bfloat16
full_type = jnp.float32


def alibi_slopes(head_count):

    def power_slopes(power_count):
        first_slope = 2.0 ** (-8.0 / power_count)
        return [first_slope ** (position + 1) for position in range(power_count)]

    nearest = 2 ** int(math.floor(math.log2(head_count)))
    slope_list = power_slopes(nearest)
    slope_list = slope_list + power_slopes(2 * nearest)[0::2][: head_count - nearest]
    return np.array(slope_list, np.float32)


def norm_stats(values):
    row_mean = jnp.mean(values, axis=-1, keepdims=True)
    centered = values - row_mean
    rstd = lax.rsqrt(jnp.mean(centered * centered, axis=-1, keepdims=True) + norm_eps)
    return centered * rstd, rstd


def norm_back(grad, unit, rstd, gain_row):
    scaled = grad * gain_row
    mean_grad = jnp.mean(scaled, axis=-1, keepdims=True)
    mean_prod = jnp.mean(scaled * unit, axis=-1, keepdims=True)
    gain_grad = jnp.sum(grad * unit, axis=0)
    shift_grad = jnp.sum(grad, axis=0)
    return rstd * (scaled - mean_grad - unit * mean_prod), gain_grad, shift_grad


def dot32(spec, left, right):
    return jnp.einsum(spec, left, right, preferred_element_type=full_type)


def two_parts(values):
    high = lax.reduce_precision(values, 8, 7)
    return high.astype(low_type), (values - high).astype(low_type)


def shards(
    tokens,
    out_grad,
    mask_pos,
    repl_id,
    replace_embed,
    masters,
    norm_params,
    first_moment,
    second_moment,
    left_basis,
    right_basis,
    norm_first,
    norm_second,
    step,
):
    seq_count = mask_pos.shape[0]
    tok_rows, width = tokens.shape
    length = tok_rows // seq_count
    heads = HEADS
    head_size = width // heads
    scale = float(head_size) ** (-0.5)
    tiles = masters.shape[0]
    ff = (tiles - 4) // 3
    rows = masters.shape[1]
    replicas = lax.axis_size("dp")
    owners = lax.axis_size("zero")
    my_copy = lax.axis_index("dp")
    my_rows = lax.axis_index("zero")

    part = rows // replicas
    shard_low = masters.astype(low_type)
    sent = lax.dynamic_slice_in_dim(shard_low, my_copy * part, part, 1)
    whole = lax.all_gather(sent, ("zero", "dp"), axis=1, tiled=True)
    norm_whole = lax.all_gather(norm_params.astype(low_type), "zero", axis=1, tiled=True)

    def outgoing(values):
        spare = owners - tiles
        return jnp.pad(values, ((0, spare),) + ((0, 0),) * (values.ndim - 1)) if spare else values

    packed = jnp.stack([left_basis, right_basis, first_moment, second_moment], axis=1)
    packed = lax.all_to_all(
        outgoing(packed.astype(low_type)), "zero", split_axis=0, concat_axis=0, tiled=True
    )
    packed = packed.transpose(1, 0, 2, 3).reshape(4, width, width)

    positions = jnp.arange(length, dtype=jnp.int32)
    mask_hits = mask_pos[:, :, None] == positions[None, None, :]
    masked = jnp.any(mask_hits, axis=1).reshape(-1, 1)
    row_ids = jnp.sum(jnp.where(mask_hits, repl_id[:, :, None], 0), axis=1).reshape(-1)
    inputs = jnp.where(masked, jnp.take(replace_embed, row_ids, axis=0), tokens)
    whole, packed, inputs = lax.optimization_barrier((whole, packed, inputs))
    left_low, right_low, moment_one_low, moment_two_low = packed
    gains = norm_whole.astype(full_type)

    slopes = jnp.asarray(alibi_slopes(heads))
    distance = jnp.abs(positions[:, None] - positions[None, :]).astype(full_type)
    alibi_bias = -slopes[:, None, None] * distance[None]
    head_shape = (seq_count, length, heads, head_size)

    qkv = [dot32("td,de->te", inputs, whole[k]).astype(low_type) for k in range(3)]
    queries, key_rows, values = [part_k.reshape(head_shape) for part_k in qkv]
    scores = dot32("bqhd,bkhd->bhqk", queries, key_rows) * scale + alibi_bias[None]
    row_max = jnp.max(scores, axis=-1, keepdims=True)
    log_total = row_max + jnp.log(jnp.sum(jnp.exp(scores - row_max), axis=-1, keepdims=True))
    probs = jnp.exp(scores - log_total)
    soft_low = probs.astype(low_type)
    mixed = dot32("bhqk,bkhd->bqhd", soft_low, values).reshape(tok_rows, width).astype(low_type)
    attended = dot32("td,de->te", mixed, whole[3])
    unit_one, rstd_one = norm_stats(inputs.astype(full_type) + attended)
    hidden = unit_one * gains[0] + gains[1]
    hidden_low = hidden.astype(low_type)

    gate = dot32("td,fde->tfe", hidden_low, whole[4 : 4 + ff])
    up = dot32("td,fde->tfe", hidden_low, whole[4 + ff : 4 + 2 * ff])
    half_erf = 0.5 + 0.5 * lax.erf(gate * math.sqrt(0.5))
    act = gate * half_erf
    slope = half_erf + gate * (jnp.exp(-0.5 * gate * gate) * (1.0 / math.sqrt(2.0 * math.pi)))
    inner_low = (act * up).astype(low_type)
    inner_low, act, up_slope = lax.optimization_barrier((inner_low, act, up * slope))
    branch = dot32("tfe,fed->td", inner_low, whole[4 + 2 * ff :])
    unit_two, rstd_two = norm_stats(hidden + branch)
    layer_out = (unit_two * gains[2] + gains[3]).astype(low_type)

    d_second, d_gain_two, d_shift_two = norm_back(
        out_grad.astype(full_type), unit_two, rstd_two, gains[2]
    )
    d_branch = d_second.astype(low_type)
    grad_down = dot32("tfe,td->fed", inner_low, d_branch).astype(low_type)
    d_inner = dot32("td,fed->tfe", d_branch, whole[4 + 2 * ff :])
    d_gate = (d_inner * up_slope).astype(low_type)
    d_up = (d_inner * act).astype(low_type)
    grad_gate = dot32("td,tfe->fde", hidden_low, d_gate).astype(low_type)
    grad_up = dot32("td,tfe->fde", hidden_low, d_up).astype(low_type)
    d_hidden = (
        d_second
        + dot32("tfe,fde->td", d_gate, whole[4 : 4 + ff])
        + dot32("tfe,fde->td", d_up, whole[4 + ff : 4 + 2 * ff])
    )
    d_first, d_gain_one, d_shift_one = norm_back(d_hidden, unit_one, rstd_one, gains[0])
    d_attended = d_first.astype(low_type)
    grad_out = dot32("td,te->de", mixed, d_attended).astype(low_type)
    d_mixed = dot32("te,de->td", d_attended, whole[3]).astype(low_type).reshape(head_shape)
    d_probs = dot32("bqhd,bkhd->bhqk", d_mixed, values)
    row_delta = jnp.sum(probs * d_probs, axis=-1, keepdims=True)
    d_scores = (probs * (d_probs - row_delta)).astype(low_type)
    d_query = dot32("bhqk,bkhd->bqhd", d_scores, key_rows) * scale
    d_keys = dot32("bhqk,bqhd->bkhd", d_scores, queries) * scale
    d_values = dot32("bhqk,bqhd->bkhd", soft_low, d_mixed)
    d_qkv = [
        grad.astype(low_type).reshape(tok_rows, width) for grad in (d_query, d_keys, d_values)
    ]
    grad_qkv = [dot32("td,te->de", inputs, grad).astype(low_type)[None] for grad in d_qkv]
    d_inputs = d_first
    for k in range(3):
        d_inputs = d_inputs + dot32("te,de->td", d_qkv[k], whole[k])
    in_grad = jnp.where(masked, 0.0, d_inputs)

    tile_grads = jnp.concatenate(
        grad_qkv + [grad_out[None], grad_gate, grad_up, grad_down], axis=0
    )
    norm_grads = jnp.stack([d_gain_one, d_shift_one, d_gain_two, d_shift_two])
    norm_sum = lax.psum(norm_grads, ("dp", "zero"))
    norm_sum = lax.dynamic_slice_in_dim(norm_sum, my_rows * norm_params.shape[1], norm_params.shape[1], 1)
    flat_grads = outgoing(tile_grads).reshape(owners * width, width)
    tile_part = lax.psum_scatter(flat_grads, ("zero", "dp"), scatter_dimension=0, tiled=True)
    tile_part, in_grad, norm_sum = lax.optimization_barrier((tile_part, in_grad, norm_sum))
    tile_sum = lax.all_gather(tile_part, "dp", axis=0, tiled=True)

    step_value = step[0].astype(full_type)
    step_rate = peak_rate * jnp.minimum(
        step_value / warm_steps, (total_steps - step_value) / (total_steps - warm_steps)
    )
    fix_one = 1.0 - jnp.power(beta_one, step_value)
    fix_two = 1.0 - jnp.power(beta_two, step_value)
    turned = dot32("ji,jl->il", left_low, tile_sum)
    high, rest = two_parts(turned)
    rotated = dot32("il,lm->im", high, right_low) + dot32("il,lm->im", rest, right_low)
    mean_one = beta_one * moment_one_low.astype(full_type) + (1.0 - beta_one) * rotated
    mean_two = beta_two * moment_two_low.astype(full_type) + (1.0 - beta_two) * rotated * rotated
    direction = mean_one / fix_one / (jnp.sqrt(mean_two / fix_two) + adam_eps)
    high, rest = two_parts(direction)
    turned = dot32("ij,jl->il", left_low, high) + dot32("ij,jl->il", left_low, rest)
    high, rest = two_parts(turned)
    update = dot32("il,ml->im", high, right_low) + dot32("il,ml->im", rest, right_low)
    results = jnp.stack(
        [rotated.astype(low_type).reshape(owners, rows, width),
         update.astype(low_type).reshape(owners, rows, width)], axis=1
    )
    returned = lax.all_to_all(results, "zero", split_axis=0, concat_axis=0, tiled=True)[:tiles]
    returned = returned.astype(full_type)
    turned_rows = returned[:, 0]
    new_first = beta_one * first_moment + (1.0 - beta_one) * turned_rows
    new_second = beta_two * second_moment + (1.0 - beta_two) * turned_rows * turned_rows
    new_master = masters - step_rate * (returned[:, 1] + decay_rate * masters)
    new_norm_first = beta_one * norm_first + (1.0 - beta_one) * norm_sum
    new_norm_second = beta_two * norm_second + (1.0 - beta_two) * norm_sum * norm_sum
    new_norms = norm_params - step_rate * (new_norm_first / fix_one) / (
        jnp.sqrt(new_norm_second / fix_two) + adam_eps
    )
    return (
        layer_out,
        in_grad,
        new_first,
        new_second,
        new_master,
        new_master.astype(low_type),
        new_norm_first,
        new_norm_second,
        new_norms,
    )


def solution(mesh):
    in_specs = (
        P(("dp", "zero"), None),
        P(("dp", "zero"), None),
        P(("dp", "zero"), None),
        P(("dp", "zero"), None),
        P(),
        P(None, "zero", None),
        P(None, "zero"),
        P(None, "zero", None),
        P(None, "zero", None),
        P(None, "zero", None),
        P(None, "zero", None),
        P(None, "zero"),
        P(None, "zero"),
        P(),
    )
    out_specs = (
        P(("dp", "zero"), None),
        P(("dp", "zero"), None),
        P(None, "zero", None),
        P(None, "zero", None),
        P(None, "zero", None),
        P(None, "zero", None),
        P(None, "zero"),
        P(None, "zero"),
        P(None, "zero"),
    )
    return jax.shard_map(shards, mesh=mesh, in_specs=in_specs, out_specs=out_specs, check_vma=False)
```

```python
import math

import jax
import jax.numpy as jnp
import numpy as np
from jax import lax
from jax.sharding import PartitionSpec as P

HEADS = 12

norm_eps = 1e-12
beta_one = 0.9
beta_two = 0.95
adam_eps = 1e-08
peak_rate = 0.1
warm_steps = 5.0
total_steps = 60.0
decay_rate = 0.01
low_type = jnp.bfloat16
full_type = jnp.float32


def alibi_slopes(head_count):

    def power_slopes(power_count):
        first_slope = 2.0 ** (-8.0 / power_count)
        return [first_slope ** (position + 1) for position in range(power_count)]

    nearest = 2 ** int(math.floor(math.log2(head_count)))
    slope_list = power_slopes(nearest)
    slope_list = slope_list + power_slopes(2 * nearest)[0::2][: head_count - nearest]
    return np.array(slope_list, np.float32)


def norm_stats(values):
    row_mean = jnp.mean(values, axis=-1, keepdims=True)
    centered = values - row_mean
    rstd = lax.rsqrt(jnp.mean(centered * centered, axis=-1, keepdims=True) + norm_eps)
    return centered * rstd, rstd


def norm_back(grad, unit, rstd, gain_row):
    scaled = grad * gain_row
    mean_grad = jnp.mean(scaled, axis=-1, keepdims=True)
    mean_prod = jnp.mean(scaled * unit, axis=-1, keepdims=True)
    gain_grad = jnp.sum(grad * unit, axis=0)
    shift_grad = jnp.sum(grad, axis=0)
    return rstd * (scaled - mean_grad - unit * mean_prod), gain_grad, shift_grad


def dot32(spec, left, right):
    return jnp.einsum(spec, left, right, preferred_element_type=full_type)


def two_parts(values):
    high = lax.reduce_precision(values, 8, 7)
    return high.astype(low_type), (values - high).astype(low_type)


def shards(
    tokens,
    out_grad,
    mask_pos,
    repl_id,
    replace_embed,
    masters,
    norm_params,
    first_moment,
    second_moment,
    left_basis,
    right_basis,
    norm_first,
    norm_second,
    step,
):
    seq_count = mask_pos.shape[0]
    tok_rows, width = tokens.shape
    length = tok_rows // seq_count
    heads = HEADS
    head_size = width // heads
    scale = float(head_size) ** (-0.5)
    tiles = masters.shape[0]
    ff = (tiles - 4) // 3
    rows = masters.shape[1]
    replicas = lax.axis_size("dp")
    owners = lax.axis_size("zero")
    my_copy = lax.axis_index("dp")
    my_rows = lax.axis_index("zero")

    part = rows // replicas
    shard_low = masters.astype(low_type)
    sent = lax.dynamic_slice_in_dim(shard_low, my_copy * part, part, 1)
    whole = lax.all_gather(sent, ("zero", "dp"), axis=1, tiled=True)
    norm_whole = lax.all_gather(norm_params.astype(low_type), "zero", axis=1, tiled=True)

    group = ff
    lines = owners // group
    my_line, my_spot = my_rows // group, my_rows % group

    def pick(values, index, axis):
        return lax.dynamic_index_in_dim(values, index, axis, keepdims=False)

    def from_copies(values, shift):
        pairs = [(i, (i + shift) % replicas) for i in range(replicas)]
        return lax.ppermute(values, "dp", pairs)

    def from_spots(values, shift):
        pairs = [(i, i - i % group + (i + shift) % group) for i in range(owners)]
        return lax.ppermute(values, "zero", pairs)

    def from_lines(values, shift, targets):
        pairs = [(i, (i + shift * group) % owners) for i in range(owners)]
        return lax.ppermute(values, "zero", [(i, k) for i, k in pairs if k // group in targets])

    def join_copies(values):
        pieces = [values] + [from_copies(values, shift) for shift in range(1, replicas)]
        if replicas == 2:
            first = my_copy == 0
            return jnp.stack(
                [jnp.where(first, pieces[0], pieces[1]), jnp.where(first, pieces[1], pieces[0])]
            )
        joined = jnp.zeros((replicas,) + values.shape, values.dtype)
        for shift, piece in enumerate(pieces):
            joined = lax.dynamic_update_index_in_dim(
                joined, piece, (my_copy + replicas - shift) % replicas, 0
            )
        return joined

    def sum_everywhere(values):
        total = values
        for shift in range(1, replicas):
            total = total + from_copies(values, shift)
        values = total
        for shift in range(1, group):
            total = total + from_spots(values, shift)
        values = total
        for shift in range(1, lines):
            total = total + from_lines(values, shift, range(lines))
        return total

    def sum_copies(tile_list):
        parts = [tile.reshape(tile.shape[:-2] + (replicas, -1, width)) for tile in tile_list]
        merge = jnp.stack if parts[0].ndim == 3 else jnp.concatenate

        def part_of(index):
            return merge([pick(tile, index, tile.ndim - 3) for tile in parts])

        total = part_of(my_copy).astype(full_type)
        for shift in range(1, replicas):
            total = total + from_copies(part_of((my_copy + shift) % replicas), shift).astype(full_type)
        return total.astype(low_type)

    def sum_spots(low):
        total = pick(low, my_spot, 0).astype(full_type)
        for shift in range(1, group):
            sent_tile = pick(low, (my_spot + shift) % group, 0)
            total = total + from_spots(sent_tile, shift).astype(full_type)
        return total.astype(low_type)

    def sum_lines(group_sums, first_line):
        last = len(group_sums) - 1
        stacked = jnp.stack(group_sums)
        targets = range(first_line, first_line + last + 1)

        def sum_for(line):
            return pick(stacked, jnp.clip(line - first_line, 0, last), 0)

        total = sum_for(my_line).astype(full_type)
        for shift in range(1, lines):
            moved = from_lines(sum_for((my_line + shift) % lines), shift, targets)
            total = total + moved.astype(full_type)
        return total

    def outgoing(values):
        spare = owners - tiles
        return jnp.pad(values, ((0, spare),) + ((0, 0),) * (values.ndim - 1)) if spare else values

    positions = jnp.arange(length, dtype=jnp.int32)
    mask_hits = mask_pos[:, :, None] == positions[None, None, :]
    masked = jnp.any(mask_hits, axis=1).reshape(-1, 1)
    row_ids = jnp.sum(jnp.where(mask_hits, repl_id[:, :, None], 0), axis=1).reshape(-1)
    inputs = jnp.where(masked, jnp.take(replace_embed, row_ids, axis=0), tokens)
    packed = jnp.stack([left_basis, right_basis, first_moment, second_moment], axis=1)
    packed = lax.dynamic_slice_in_dim(packed, my_copy * part, part, 2).astype(low_type)
    whole, inputs, packed = lax.optimization_barrier((whole, inputs, outgoing(packed)))
    packed = lax.all_to_all(packed, "zero", split_axis=0, concat_axis=0, tiled=True)
    gains = norm_whole.astype(full_type)

    slopes = jnp.asarray(alibi_slopes(heads))
    distance = jnp.abs(positions[:, None] - positions[None, :]).astype(full_type)
    alibi_bias = -slopes[:, None, None] * distance[None]
    head_shape = (seq_count, length, heads, head_size)

    qkv = [dot32("td,de->te", inputs, whole[k]).astype(low_type) for k in range(3)]
    queries, key_rows, values = [part_k.reshape(head_shape) for part_k in qkv]
    scores = dot32("bqhd,bkhd->bhqk", queries, key_rows) * scale + alibi_bias[None]
    row_max = jnp.max(scores, axis=-1, keepdims=True)
    log_total = row_max + jnp.log(jnp.sum(jnp.exp(scores - row_max), axis=-1, keepdims=True))
    probs = jnp.exp(scores - log_total)
    soft_low = probs.astype(low_type)
    mixed = dot32("bhqk,bkhd->bqhd", soft_low, values).reshape(tok_rows, width).astype(low_type)
    attended = dot32("td,de->te", mixed, whole[3])
    unit_one, rstd_one = norm_stats(inputs.astype(full_type) + attended)
    hidden = unit_one * gains[0] + gains[1]
    hidden_low = hidden.astype(low_type)

    gate = dot32("td,fde->tfe", hidden_low, whole[4 : 4 + ff])
    up = dot32("td,fde->tfe", hidden_low, whole[4 + ff : 4 + 2 * ff])
    half_erf = 0.5 + 0.5 * lax.erf(gate * math.sqrt(0.5))
    act = gate * half_erf
    slope = half_erf + gate * (jnp.exp(-0.5 * gate * gate) * (1.0 / math.sqrt(2.0 * math.pi)))
    inner_low = (act * up).astype(low_type)
    inner_low, act, up_slope = lax.optimization_barrier((inner_low, act, up * slope))
    branch = dot32("tfe,fed->td", inner_low, whole[4 + 2 * ff :])
    branch, packed = lax.optimization_barrier((branch, packed))
    unit_two, rstd_two = norm_stats(hidden + branch)
    layer_out = (unit_two * gains[2] + gains[3]).astype(low_type)

    d_second, d_gain_two, d_shift_two = norm_back(
        out_grad.astype(full_type), unit_two, rstd_two, gains[2]
    )
    d_branch = d_second.astype(low_type)
    grad_down = dot32("tfe,td->fed", inner_low, d_branch).astype(low_type)
    d_branch, grad_down = lax.optimization_barrier((d_branch, grad_down))
    down_low = sum_copies([grad_down])
    packed = join_copies(packed)
    d_inner = dot32("td,fed->tfe", d_branch, whole[4 + 2 * ff :])
    d_gate = (d_inner * up_slope).astype(low_type)
    d_up = (d_inner * act).astype(low_type)
    d_gate, d_up, down_low, packed = lax.optimization_barrier((d_gate, d_up, down_low, packed))
    down_sum = sum_spots(down_low)
    grad_gate = dot32("td,tfe->fde", hidden_low, d_gate).astype(low_type)
    grad_up = dot32("td,tfe->fde", hidden_low, d_up).astype(low_type)
    d_gate, d_up, grad_gate, grad_up, down_sum = lax.optimization_barrier(
        (d_gate, d_up, grad_gate, grad_up, down_sum)
    )
    gate_low = sum_copies([grad_gate])
    up_low = sum_copies([grad_up])
    d_hidden = (
        d_second
        + dot32("tfe,fde->td", d_gate, whole[4 : 4 + ff])
        + dot32("tfe,fde->td", d_up, whole[4 + ff : 4 + 2 * ff])
    )
    d_hidden, gate_low, up_low = lax.optimization_barrier((d_hidden, gate_low, up_low))
    gate_sum = sum_spots(gate_low)
    up_sum = sum_spots(up_low)
    d_first, d_gain_one, d_shift_one = norm_back(d_hidden, unit_one, rstd_one, gains[0])
    d_attended = d_first.astype(low_type)
    grad_out = dot32("td,te->de", mixed, d_attended).astype(low_type)
    d_mixed = dot32("te,de->td", d_attended, whole[3]).astype(low_type).reshape(head_shape)
    d_probs = dot32("bqhd,bkhd->bhqk", d_mixed, values)
    row_delta = jnp.sum(probs * d_probs, axis=-1, keepdims=True)
    d_scores = (probs * (d_probs - row_delta)).astype(low_type)
    d_scores, gate_sum, up_sum = lax.optimization_barrier((d_scores, gate_sum, up_sum))
    ff_total = sum_lines([gate_sum, up_sum, down_sum], 1)
    norm_sum = sum_everywhere(jnp.stack([d_gain_one, d_shift_one, d_gain_two, d_shift_two]))
    d_query = dot32("bhqk,bkhd->bqhd", d_scores, key_rows) * scale
    d_keys = dot32("bhqk,bqhd->bkhd", d_scores, queries) * scale
    d_values = dot32("bhqk,bqhd->bkhd", soft_low, d_mixed)
    d_qkv = [
        grad.astype(low_type).reshape(tok_rows, width) for grad in (d_query, d_keys, d_values)
    ]
    *d_qkv, norm_sum = lax.optimization_barrier((*d_qkv, norm_sum))
    grad_qkv = [dot32("td,te->de", inputs, grad).astype(low_type) for grad in d_qkv]
    d_inputs = d_first
    for k in range(3):
        d_inputs = d_inputs + dot32("te,de->td", d_qkv[k], whole[k])
    in_grad = jnp.where(masked, 0.0, d_inputs)

    columns = norm_params.shape[1]
    norm_sum = lax.dynamic_slice_in_dim(norm_sum, my_rows * columns, columns, 1)
    *grad_qkv, ff_total = lax.optimization_barrier((*grad_qkv, ff_total))
    attention_low = sum_copies(grad_qkv + [grad_out])
    attention_total = sum_lines([sum_spots(attention_low)], 0)
    mine = jnp.where(my_line == 0, attention_total, ff_total).astype(low_type)
    tile_sum = join_copies(mine).reshape(width, width)
    packed = packed.transpose(2, 1, 0, 3, 4).reshape(4, width, width)
    left_low, right_low, moment_one_low, moment_two_low = packed

    step_value = step[0].astype(full_type)
    step_rate = peak_rate * jnp.minimum(
        step_value / warm_steps, (total_steps - step_value) / (total_steps - warm_steps)
    )
    fix_one = 1.0 - jnp.power(beta_one, step_value)
    fix_two = 1.0 - jnp.power(beta_two, step_value)
    turned = dot32("ji,jl->il", left_low, tile_sum)
    high, rest = two_parts(turned)
    rotated = dot32("il,lm->im", high, right_low) + dot32("il,lm->im", rest, right_low)
    mean_one = beta_one * moment_one_low.astype(full_type) + (1.0 - beta_one) * rotated
    mean_two = beta_two * moment_two_low.astype(full_type) + (1.0 - beta_two) * rotated * rotated
    direction = mean_one / fix_one / (jnp.sqrt(mean_two / fix_two) + adam_eps)
    high, rest = two_parts(direction)
    turned = dot32("ij,jl->il", left_low, high) + dot32("ij,jl->il", left_low, rest)
    high, rest = two_parts(turned)
    update = dot32("il,ml->im", high, right_low) + dot32("il,ml->im", rest, right_low)
    results = jnp.stack([rotated, update]).reshape(2, owners, replicas, part, width)
    results = pick(results, my_copy, 2).astype(low_type).transpose(1, 0, 2, 3)
    returned = lax.all_to_all(results, "zero", split_axis=0, concat_axis=0, tiled=True)[:tiles]
    returned = join_copies(returned).transpose(1, 2, 0, 3, 4)
    returned = returned.reshape(tiles, 2, rows, width).astype(full_type)
    turned_rows = returned[:, 0]
    new_first = beta_one * first_moment + (1.0 - beta_one) * turned_rows
    new_second = beta_two * second_moment + (1.0 - beta_two) * turned_rows * turned_rows
    new_master = masters - step_rate * (returned[:, 1] + decay_rate * masters)
    new_norm_first = beta_one * norm_first + (1.0 - beta_one) * norm_sum
    new_norm_second = beta_two * norm_second + (1.0 - beta_two) * norm_sum * norm_sum
    new_norms = norm_params - step_rate * (new_norm_first / fix_one) / (
        jnp.sqrt(new_norm_second / fix_two) + adam_eps
    )
    return (
        layer_out,
        in_grad,
        new_first,
        new_second,
        new_master,
        new_master.astype(low_type),
        new_norm_first,
        new_norm_second,
        new_norms,
    )


def solution(mesh):
    in_specs = (
        P(("dp", "zero"), None),
        P(("dp", "zero"), None),
        P(("dp", "zero"), None),
        P(("dp", "zero"), None),
        P(),
        P(None, "zero", None),
        P(None, "zero"),
        P(None, "zero", None),
        P(None, "zero", None),
        P(None, "zero", None),
        P(None, "zero", None),
        P(None, "zero"),
        P(None, "zero"),
        P(),
    )
    out_specs = (
        P(("dp", "zero"), None),
        P(("dp", "zero"), None),
        P(None, "zero", None),
        P(None, "zero", None),
        P(None, "zero", None),
        P(None, "zero", None),
        P(None, "zero"),
        P(None, "zero"),
        P(None, "zero"),
    )
    return jax.shard_map(shards, mesh=mesh, in_specs=in_specs, out_specs=out_specs, check_vma=False)
```

```python
import math

import jax
import jax.numpy as jnp
import numpy as np
from jax import lax
from jax.sharding import PartitionSpec as P


HEADS = 12

norm_eps = 1e-12
beta_one = 0.9
beta_two = 0.95
adam_eps = 1e-08
peak_rate = 0.1
warm_steps = 5.0
total_steps = 60.0
decay_rate = 0.01
low_type = jnp.bfloat16
full_type = jnp.float32


def alibi_slopes(head_count):

    def power_slopes(power_count):
        first_slope = 2.0 ** (-8.0 / power_count)
        return [first_slope ** (position + 1) for position in range(power_count)]

    nearest = 2 ** int(math.floor(math.log2(head_count)))
    slope_list = power_slopes(nearest)
    slope_list = slope_list + power_slopes(2 * nearest)[0::2][: head_count - nearest]
    return np.array(slope_list, np.float32)


def norm_stats(values):
    row_mean = jnp.mean(values, axis=-1, keepdims=True)
    centered = values - row_mean
    rstd = lax.rsqrt(jnp.mean(centered * centered, axis=-1, keepdims=True) + norm_eps)
    return centered * rstd, rstd


def norm_back(grad, unit, rstd, gain_row):
    scaled = grad * gain_row
    mean_grad = jnp.mean(scaled, axis=-1, keepdims=True)
    mean_prod = jnp.mean(scaled * unit, axis=-1, keepdims=True)
    gain_grad = jnp.sum(grad * unit, axis=0)
    shift_grad = jnp.sum(grad, axis=0)
    return rstd * (scaled - mean_grad - unit * mean_prod), gain_grad, shift_grad


def dot32(spec, left, right):
    return jnp.einsum(spec, left, right, preferred_element_type=full_type)


def two_parts(values):
    high = lax.reduce_precision(values, 8, 7)
    return high.astype(low_type), (values - high).astype(low_type)


def shards(
    tokens,
    out_grad,
    mask_pos,
    repl_id,
    replace_embed,
    masters,
    norm_params,
    first_moment,
    second_moment,
    left_basis,
    right_basis,
    norm_first,
    norm_second,
    step,
):
    seq_count = mask_pos.shape[0]
    tok_rows, width = tokens.shape
    length = tok_rows // seq_count
    heads = HEADS
    head_size = width // heads
    scale = float(head_size) ** (-0.5)
    tiles = masters.shape[0]
    ff = (tiles - 4) // 3
    rows = masters.shape[1]
    replicas = lax.axis_size("dp")
    owners = lax.axis_size("zero")
    my_copy = lax.axis_index("dp")
    my_rows = lax.axis_index("zero")

    part = rows // replicas
    shard_low = masters.astype(low_type)
    sent = lax.dynamic_slice_in_dim(shard_low, my_copy * part, part, 1)
    whole = lax.all_gather(sent, ("zero", "dp"), axis=1, tiled=True)
    norm_whole = lax.all_gather(norm_params.astype(low_type), "zero", axis=1, tiled=True)

    group = ff
    lines = owners // group
    my_line, my_spot = my_rows // group, my_rows % group

    def pick(values, index, axis):
        return lax.dynamic_index_in_dim(values, index, axis, keepdims=False)

    def from_copies(values, shift):
        pairs = [(i, (i + shift) % replicas) for i in range(replicas)]
        return lax.ppermute(values, "dp", pairs)

    def from_spots(values, shift):
        pairs = [(i, i - i % group + (i + shift) % group) for i in range(owners)]
        return lax.ppermute(values, "zero", pairs)

    def from_lines(values, shift):
        pairs = [(i, (i + shift * group) % owners) for i in range(owners)]
        return lax.ppermute(values, "zero", pairs)

    def from_line(values, line, shift):
        pairs = [(i, (i + shift * group) % owners) for i in range(owners) if i // group == line]
        return lax.ppermute(values, "zero", pairs)

    def join_copies(values):
        pieces = [values] + [from_copies(values, shift) for shift in range(1, replicas)]
        if replicas == 2:
            first = my_copy == 0
            return jnp.stack(
                [jnp.where(first, pieces[0], pieces[1]), jnp.where(first, pieces[1], pieces[0])]
            )
        joined = jnp.zeros((replicas,) + values.shape, values.dtype)
        for shift, piece in enumerate(pieces):
            joined = lax.dynamic_update_index_in_dim(
                joined, piece, (my_copy + replicas - shift) % replicas, 0
            )
        return joined

    def sum_everywhere(values):
        total = values
        for shift in range(1, replicas):
            total = total + from_copies(values, shift)
        values = total
        for shift in range(1, group):
            total = total + from_spots(values, shift)
        values = total
        for shift in range(1, lines):
            total = total + from_lines(values, shift)
        return total

    def sum_copies(tile_list):
        parts = [tile.reshape(tile.shape[:-2] + (replicas, -1, width)) for tile in tile_list]
        merge = jnp.stack if parts[0].ndim == 3 else jnp.concatenate

        def part_of(index):
            return merge([pick(tile, index, tile.ndim - 3) for tile in parts])

        total = part_of(my_copy).astype(full_type)
        for shift in range(1, replicas):
            total = total + from_copies(part_of((my_copy + shift) % replicas), shift).astype(full_type)
        return total.astype(low_type)

    def sum_spots(low):
        total = pick(low, my_spot, 0).astype(full_type)
        for shift in range(1, group):
            sent_tile = pick(low, (my_spot + shift) % group, 0)
            moved = from_spots(sent_tile, shift)
            total = total + moved.astype(full_type)
        return total.astype(low_type)

    def sum_lines(low, target):
        total = low.astype(full_type)
        for shift in range(1, lines):
            moved = from_line(low, (target - shift) % lines, shift)
            total = total + moved.astype(full_type)
        return total

    def outgoing(values):
        values = jnp.concatenate([values[tiles - group :], values[: tiles - group]])
        spare = owners - tiles
        return jnp.pad(values, ((0, spare),) + ((0, 0),) * (values.ndim - 1)) if spare else values

    positions = jnp.arange(length, dtype=jnp.int32)
    mask_hits = mask_pos[:, :, None] == positions[None, None, :]
    masked = jnp.any(mask_hits, axis=1).reshape(-1, 1)
    row_ids = jnp.sum(jnp.where(mask_hits, repl_id[:, :, None], 0), axis=1).reshape(-1)
    inputs = jnp.where(masked, jnp.take(replace_embed, row_ids, axis=0), tokens)
    packed = jnp.stack([left_basis, right_basis, first_moment, second_moment], axis=1)
    packed = lax.dynamic_slice_in_dim(packed, my_copy * part, part, 2).astype(low_type)
    whole, inputs, packed = lax.optimization_barrier((whole, inputs, outgoing(packed)))
    packed = lax.all_to_all(packed, "zero", split_axis=0, concat_axis=0, tiled=True)
    gains = norm_whole.astype(full_type)

    slopes = jnp.asarray(alibi_slopes(heads))
    distance = jnp.abs(positions[:, None] - positions[None, :]).astype(full_type)
    alibi_bias = -slopes[:, None, None] * distance[None]
    head_shape = (seq_count, length, heads, head_size)

    qkv = [dot32("td,de->te", inputs, whole[k]).astype(low_type) for k in range(3)]
    queries, key_rows, values = [part_k.reshape(head_shape) for part_k in qkv]
    scores = dot32("bqhd,bkhd->bhqk", queries, key_rows) * scale + alibi_bias[None]
    row_max = jnp.max(scores, axis=-1, keepdims=True)
    log_total = row_max + jnp.log(jnp.sum(jnp.exp(scores - row_max), axis=-1, keepdims=True))
    probs = jnp.exp(scores - log_total)
    soft_low = probs.astype(low_type)
    mixed = dot32("bhqk,bkhd->bqhd", soft_low, values).reshape(tok_rows, width).astype(low_type)
    attended = dot32("td,de->te", mixed, whole[3])
    unit_one, rstd_one = norm_stats(inputs.astype(full_type) + attended)
    hidden = unit_one * gains[0] + gains[1]
    hidden_low = hidden.astype(low_type)

    gate = dot32("td,fde->tfe", hidden_low, whole[4 : 4 + ff])
    up = dot32("td,fde->tfe", hidden_low, whole[4 + ff : 4 + 2 * ff])
    half_erf = 0.5 + 0.5 * lax.erf(gate * math.sqrt(0.5))
    act = gate * half_erf
    slope = half_erf + gate * (jnp.exp(-0.5 * gate * gate) * (1.0 / math.sqrt(2.0 * math.pi)))
    inner_low = (act * up).astype(low_type)
    inner_low, act, up_slope = lax.optimization_barrier((inner_low, act, up * slope))
    branch = dot32("tfe,fed->td", inner_low, whole[4 + 2 * ff :])
    branch, packed = lax.optimization_barrier((branch, packed))
    unit_two, rstd_two = norm_stats(hidden + branch)
    layer_out = (unit_two * gains[2] + gains[3]).astype(low_type)

    d_second, d_gain_two, d_shift_two = norm_back(
        out_grad.astype(full_type), unit_two, rstd_two, gains[2]
    )
    d_branch = d_second.astype(low_type)
    grad_down = [
        dot32("te,td->ed", inner_low[:, f], d_branch).astype(low_type) for f in range(ff)
    ]
    d_branch, grad_down = lax.optimization_barrier((d_branch, grad_down))
    down_low = sum_copies(grad_down)
    packed = join_copies(packed)
    d_inner = dot32("td,fed->tfe", d_branch, whole[4 + 2 * ff :])
    d_gate = (d_inner * up_slope).astype(low_type)
    d_up = (d_inner * act).astype(low_type)
    d_gate, d_up, down_low, packed = lax.optimization_barrier((d_gate, d_up, down_low, packed))
    down_sum = sum_spots(down_low)
    grad_gate = [dot32("td,te->de", hidden_low, d_gate[:, f]).astype(low_type) for f in range(ff)]
    grad_up = [dot32("td,te->de", hidden_low, d_up[:, f]).astype(low_type) for f in range(ff)]
    d_gate, d_up, grad_gate, grad_up, down_sum = lax.optimization_barrier(
        (d_gate, d_up, grad_gate, grad_up, down_sum)
    )
    gate_low = sum_copies(grad_gate)
    up_low = sum_copies(grad_up)
    d_hidden = (
        d_second
        + dot32("tfe,fde->td", d_gate, whole[4 : 4 + ff])
        + dot32("tfe,fde->td", d_up, whole[4 + ff : 4 + 2 * ff])
    )
    d_hidden, gate_low, up_low = lax.optimization_barrier((d_hidden, gate_low, up_low))
    down_total = sum_lines(down_sum, 0)
    gate_sum = sum_spots(gate_low)
    up_sum = sum_spots(up_low)
    gate_total = sum_lines(gate_sum, 2)
    up_total = sum_lines(up_sum, 3)
    d_first, d_gain_one, d_shift_one = norm_back(d_hidden, unit_one, rstd_one, gains[0])
    d_attended = d_first.astype(low_type)
    grad_out = dot32("td,te->de", mixed, d_attended).astype(low_type)
    d_mixed = dot32("te,de->td", d_attended, whole[3]).astype(low_type).reshape(head_shape)
    d_probs = dot32("bqhd,bkhd->bhqk", d_mixed, values)
    row_delta = jnp.sum(probs * d_probs, axis=-1, keepdims=True)
    d_scores = (probs * (d_probs - row_delta)).astype(low_type)
    norm_sum = sum_everywhere(jnp.stack([d_gain_one, d_shift_one, d_gain_two, d_shift_two]))
    d_query = dot32("bhqk,bkhd->bqhd", d_scores, key_rows) * scale
    d_keys = dot32("bhqk,bqhd->bkhd", d_scores, queries) * scale
    d_values = dot32("bhqk,bqhd->bkhd", soft_low, d_mixed)
    d_qkv = [
        grad.astype(low_type).reshape(tok_rows, width) for grad in (d_query, d_keys, d_values)
    ]
    grad_values = dot32("td,te->de", inputs, d_qkv[2]).astype(low_type)
    grad_keys = dot32("td,te->de", inputs, d_qkv[1]).astype(low_type)
    grad_query = dot32("td,te->de", inputs, d_qkv[0]).astype(low_type)
    grad_qkv = [grad_query, grad_keys, grad_values]
    d_inputs = d_first
    for k in range(3):
        d_inputs = d_inputs + dot32("te,de->td", d_qkv[k], whole[k])
    in_grad = jnp.where(masked, 0.0, d_inputs)

    columns = norm_params.shape[1]
    norm_sum = lax.dynamic_slice_in_dim(norm_sum, my_rows * columns, columns, 1)
    attention_low = sum_copies(grad_qkv + [grad_out])
    mine = sum_lines(sum_spots(attention_low), 1)
    mine, norm_sum = lax.optimization_barrier((mine, norm_sum))
    mine = jnp.where(my_line == 0, down_total, mine)
    mine = jnp.where(my_line == 2, gate_total, mine)
    mine = jnp.where(my_line == 3, up_total, mine).astype(low_type)
    tile_sum = join_copies(mine).reshape(width, width)
    packed = packed.transpose(2, 1, 0, 3, 4).reshape(4, width, width)
    left_low, right_low, moment_one_low, moment_two_low = packed

    step_value = step[0].astype(full_type)
    step_rate = peak_rate * jnp.minimum(
        step_value / warm_steps, (total_steps - step_value) / (total_steps - warm_steps)
    )
    fix_one = 1.0 - jnp.power(beta_one, step_value)
    fix_two = 1.0 - jnp.power(beta_two, step_value)
    turned = dot32("ji,jl->il", left_low, tile_sum)
    high, rest = two_parts(turned)
    rotated = dot32("il,lm->im", high, right_low) + dot32("il,lm->im", rest, right_low)
    mean_one = beta_one * moment_one_low.astype(full_type) + (1.0 - beta_one) * rotated
    mean_two = beta_two * moment_two_low.astype(full_type) + (1.0 - beta_two) * rotated * rotated
    direction = mean_one / fix_one / (jnp.sqrt(mean_two / fix_two) + adam_eps)
    high, rest = two_parts(direction)
    turned = dot32("ij,jl->il", left_low, high) + dot32("ij,jl->il", left_low, rest)
    high, rest = two_parts(turned)
    update = dot32("il,ml->im", high, right_low) + dot32("il,ml->im", rest, right_low)
    results = jnp.stack([rotated, update]).reshape(2, owners, replicas, part, width)
    results = pick(results, my_copy, 2).astype(low_type).transpose(1, 0, 2, 3)
    returned = lax.all_to_all(results, "zero", split_axis=0, concat_axis=0, tiled=True)
    returned = jnp.concatenate([returned[group:tiles], returned[:group]])
    returned = join_copies(returned).transpose(1, 2, 0, 3, 4)
    returned = returned.reshape(tiles, 2, rows, width).astype(full_type)
    turned_rows = returned[:, 0]
    new_first = beta_one * first_moment + (1.0 - beta_one) * turned_rows
    new_second = beta_two * second_moment + (1.0 - beta_two) * turned_rows * turned_rows
    new_master = masters - step_rate * (returned[:, 1] + decay_rate * masters)
    new_norm_first = beta_one * norm_first + (1.0 - beta_one) * norm_sum
    new_norm_second = beta_two * norm_second + (1.0 - beta_two) * norm_sum * norm_sum
    new_norms = norm_params - step_rate * (new_norm_first / fix_one) / (
        jnp.sqrt(new_norm_second / fix_two) + adam_eps
    )
    return (
        layer_out,
        in_grad,
        new_first,
        new_second,
        new_master,
        new_master.astype(low_type),
        new_norm_first,
        new_norm_second,
        new_norms,
    )


def solution(mesh):
    in_specs = (
        P(("dp", "zero"), None),
        P(("dp", "zero"), None),
        P(("dp", "zero"), None),
        P(("dp", "zero"), None),
        P(),
        P(None, "zero", None),
        P(None, "zero"),
        P(None, "zero", None),
        P(None, "zero", None),
        P(None, "zero", None),
        P(None, "zero", None),
        P(None, "zero"),
        P(None, "zero"),
        P(),
    )
    out_specs = (
        P(("dp", "zero"), None),
        P(("dp", "zero"), None),
        P(None, "zero", None),
        P(None, "zero", None),
        P(None, "zero", None),
        P(None, "zero", None),
        P(None, "zero"),
        P(None, "zero"),
        P(None, "zero"),
    )
    return jax.shard_map(shards, mesh=mesh, in_specs=in_specs, out_specs=out_specs, check_vma=False)
```

```python
import math

import jax
import jax.numpy as jnp
import numpy as np
from jax import lax
from jax.sharding import PartitionSpec as P


HEADS = 12

norm_eps = 1e-12
beta_one = 0.9
beta_two = 0.95
adam_eps = 1e-08
peak_rate = 0.1
warm_steps = 5.0
total_steps = 60.0
decay_rate = 0.01
low_type = jnp.bfloat16
full_type = jnp.float32


def alibi_slopes(head_count):

    def power_slopes(power_count):
        first_slope = 2.0 ** (-8.0 / power_count)
        return [first_slope ** (position + 1) for position in range(power_count)]

    nearest = 2 ** int(math.floor(math.log2(head_count)))
    slope_list = power_slopes(nearest)
    slope_list = slope_list + power_slopes(2 * nearest)[0::2][: head_count - nearest]
    return np.array(slope_list, np.float32)


def norm_stats(values):
    row_mean = jnp.mean(values, axis=-1, keepdims=True)
    centered = values - row_mean
    rstd = lax.rsqrt(jnp.mean(centered * centered, axis=-1, keepdims=True) + norm_eps)
    return centered * rstd, rstd


def norm_back(grad, unit, rstd, gain_row):
    scaled = grad * gain_row
    mean_grad = jnp.mean(scaled, axis=-1, keepdims=True)
    mean_prod = jnp.mean(scaled * unit, axis=-1, keepdims=True)
    gain_grad = jnp.sum(grad * unit, axis=0)
    shift_grad = jnp.sum(grad, axis=0)
    return rstd * (scaled - mean_grad - unit * mean_prod), gain_grad, shift_grad


def dot32(spec, left, right):
    return jnp.einsum(spec, left, right, preferred_element_type=full_type)


def two_parts(values):
    high = lax.reduce_precision(values, 8, 7)
    return high.astype(low_type), (values - high).astype(low_type)


def shards(
    tokens,
    out_grad,
    mask_pos,
    repl_id,
    replace_embed,
    masters,
    norm_params,
    first_moment,
    second_moment,
    left_basis,
    right_basis,
    norm_first,
    norm_second,
    step,
):
    seq_count = mask_pos.shape[0]
    tok_rows, width = tokens.shape
    length = tok_rows // seq_count
    heads = HEADS
    head_size = width // heads
    scale = float(head_size) ** (-0.5)
    tiles = masters.shape[0]
    ff = (tiles - 4) // 3
    rows = masters.shape[1]
    replicas = lax.axis_size("dp")
    owners = lax.axis_size("zero")
    my_copy = lax.axis_index("dp")
    my_rows = lax.axis_index("zero")

    part = rows // replicas
    shard_low = masters.astype(low_type)
    sent = lax.dynamic_slice_in_dim(shard_low, my_copy * part, part, 1)

    group = ff
    lines = owners // group
    my_line, my_spot = my_rows // group, my_rows % group

    def pick(values, index, axis):
        return lax.dynamic_index_in_dim(values, index, axis, keepdims=False)

    def from_copies(values, shift):
        pairs = [(i, (i + shift) % replicas) for i in range(replicas)]
        return lax.ppermute(values, "dp", pairs)

    def from_spots(values, shift):
        pairs = [(i, i - i % group + (i + shift) % group) for i in range(owners)]
        return lax.ppermute(values, "zero", pairs)

    def from_lines(values, shift):
        pairs = [(i, (i + shift * group) % owners) for i in range(owners)]
        return lax.ppermute(values, "zero", pairs)

    def from_line(values, line, shift):
        pairs = [(i, (i + shift * group) % owners) for i in range(owners) if i // group == line]
        return lax.ppermute(values, "zero", pairs)

    def join_copies(values):
        pieces = [values] + [from_copies(values, shift) for shift in range(1, replicas)]
        if replicas == 2:
            first = my_copy == 0
            return jnp.stack(
                [jnp.where(first, pieces[0], pieces[1]), jnp.where(first, pieces[1], pieces[0])]
            )
        joined = jnp.zeros((replicas,) + values.shape, values.dtype)
        for shift, piece in enumerate(pieces):
            joined = lax.dynamic_update_index_in_dim(
                joined, piece, (my_copy + replicas - shift) % replicas, 0
            )
        return joined

    def place(pieces, me, axis):
        count = len(pieces)
        shape = list(pieces[0].shape)
        shape.insert(axis, count)
        placed = jnp.zeros(shape, pieces[0].dtype)
        for shift, piece in enumerate(pieces):
            index = (me + count - shift) % count
            placed = lax.dynamic_update_index_in_dim(placed, piece, index, axis)
        return placed

    def gather_rows(values):
        pieces = [values]
        for shift in range(1, lines):
            pieces.append(from_lines(values, shift))
        values = place(pieces, my_line, 1)
        pieces = [values]
        for shift in range(1, group):
            pieces.append(from_spots(values, shift))
        return place(pieces, my_spot, 2)

    def gather_tiles(values):
        half = gather_rows(values)
        pieces = [half]
        for shift in range(1, replicas):
            pieces.append(from_copies(half, shift))
        if replicas == 2:
            first = my_copy == 0
            joined = jnp.stack(
                [jnp.where(first, pieces[0], pieces[1]), jnp.where(first, pieces[1], pieces[0])],
                axis=3,
            )
        else:
            joined = place(pieces, my_copy, 3)
        return joined.reshape(values.shape[0], width, width)

    def sum_everywhere(values):
        total = values
        for shift in range(1, replicas):
            total = total + from_copies(values, shift)
        values = total
        for shift in range(1, group):
            total = total + from_spots(values, shift)
        values = total
        for shift in range(1, lines):
            total = total + from_lines(values, shift)
        return total

    def sum_copies(tile_list):
        parts = [tile.reshape(tile.shape[:-2] + (replicas, -1, width)) for tile in tile_list]
        merge = jnp.stack if parts[0].ndim == 3 else jnp.concatenate

        def part_of(index):
            return merge([pick(tile, index, tile.ndim - 3) for tile in parts])

        total = part_of(my_copy).astype(full_type)
        for shift in range(1, replicas):
            total = total + from_copies(part_of((my_copy + shift) % replicas), shift).astype(full_type)
        return total.astype(low_type)

    def sum_spots(low):
        total = pick(low, my_spot, 0).astype(full_type)
        for shift in range(1, group):
            sent_tile = pick(low, (my_spot + shift) % group, 0)
            moved = from_spots(sent_tile, shift)
            total = total + moved.astype(full_type)
        return total.astype(low_type)

    def sum_lines(low, target):
        total = low.astype(full_type)
        for shift in range(1, lines):
            moved = from_line(low, (target - shift) % lines, shift)
            total = total + moved.astype(full_type)
        return total

    def outgoing(values):
        values = jnp.concatenate([values[tiles - group :], values[: tiles - group]])
        spare = owners - tiles
        return jnp.pad(values, ((0, spare),) + ((0, 0),) * (values.ndim - 1)) if spare else values

    positions = jnp.arange(length, dtype=jnp.int32)
    mask_hits = mask_pos[:, :, None] == positions[None, None, :]
    masked = jnp.any(mask_hits, axis=1).reshape(-1, 1)
    row_ids = jnp.sum(jnp.where(mask_hits, repl_id[:, :, None], 0), axis=1).reshape(-1)
    inputs = jnp.where(masked, jnp.take(replace_embed, row_ids, axis=0), tokens)
    attention_w = gather_tiles(sent[:4])
    gate_w = gather_tiles(sent[4 : 4 + ff])
    up_w = gather_tiles(sent[4 + ff : 4 + 2 * ff])
    down_w = gather_tiles(sent[4 + 2 * ff :])
    norm_low = norm_params.astype(low_type)[:, None, :]
    gains = gather_rows(norm_low).reshape(norm_params.shape[0], width)
    attention_w, inputs, gains = lax.optimization_barrier((attention_w, inputs, gains))
    gains = gains.astype(full_type)

    slopes = jnp.asarray(alibi_slopes(heads))
    distance = jnp.abs(positions[:, None] - positions[None, :]).astype(full_type)
    alibi_bias = -slopes[:, None, None] * distance[None]
    head_shape = (seq_count, length, heads, head_size)

    qkv = [dot32("td,de->te", inputs, attention_w[k]).astype(low_type) for k in range(3)]
    queries, key_rows, values = [part_k.reshape(head_shape) for part_k in qkv]
    scores = dot32("bqhd,bkhd->bhqk", queries, key_rows) * scale + alibi_bias[None]
    row_max = jnp.max(scores, axis=-1, keepdims=True)
    log_total = row_max + jnp.log(jnp.sum(jnp.exp(scores - row_max), axis=-1, keepdims=True))
    probs = jnp.exp(scores - log_total)
    soft_low = probs.astype(low_type)
    mixed = dot32("bhqk,bkhd->bqhd", soft_low, values).reshape(tok_rows, width).astype(low_type)
    attended = dot32("td,de->te", mixed, attention_w[3])
    unit_one, rstd_one = norm_stats(inputs.astype(full_type) + attended)
    hidden = unit_one * gains[0] + gains[1]
    hidden_low = hidden.astype(low_type)

    gate = dot32("td,fde->tfe", hidden_low, gate_w)
    up = dot32("td,fde->tfe", hidden_low, up_w)
    half_erf = 0.5 + 0.5 * lax.erf(gate * math.sqrt(0.5))
    act = gate * half_erf
    slope = half_erf + gate * (jnp.exp(-0.5 * gate * gate) * (1.0 / math.sqrt(2.0 * math.pi)))
    inner_low = (act * up).astype(low_type)
    inner_low, act, up_slope = lax.optimization_barrier((inner_low, act, up * slope))
    branch = dot32("tfe,fed->td", inner_low, down_w)
    packed = jnp.stack([left_basis, right_basis, first_moment, second_moment], axis=1)
    packed = lax.dynamic_slice_in_dim(packed, my_copy * part, part, 2).astype(low_type)
    branch, packed = lax.optimization_barrier((branch, outgoing(packed)))
    packed = lax.all_to_all(packed, "zero", split_axis=0, concat_axis=0, tiled=True)
    unit_two, rstd_two = norm_stats(hidden + branch)
    layer_out = (unit_two * gains[2] + gains[3]).astype(low_type)

    d_second, d_gain_two, d_shift_two = norm_back(
        out_grad.astype(full_type), unit_two, rstd_two, gains[2]
    )
    d_branch = d_second.astype(low_type)
    grad_down = [
        dot32("te,td->ed", inner_low[:, f], d_branch).astype(low_type) for f in range(ff)
    ]
    d_branch, grad_down = lax.optimization_barrier((d_branch, grad_down))
    down_low = sum_copies(grad_down)
    d_inner = dot32("td,fed->tfe", d_branch, down_w)
    d_gate = (d_inner * up_slope).astype(low_type)
    d_up = (d_inner * act).astype(low_type)
    d_gate, d_up, down_low, packed = lax.optimization_barrier((d_gate, d_up, down_low, packed))
    packed = join_copies(packed)
    down_sum = sum_spots(down_low)
    grad_gate = [dot32("td,te->de", hidden_low, d_gate[:, f]).astype(low_type) for f in range(ff)]
    grad_up = [dot32("td,te->de", hidden_low, d_up[:, f]).astype(low_type) for f in range(ff)]
    d_gate, d_up, grad_gate, grad_up, down_sum = lax.optimization_barrier(
        (d_gate, d_up, grad_gate, grad_up, down_sum)
    )
    gate_low = sum_copies(grad_gate)
    up_low = sum_copies(grad_up)
    d_hidden = (
        d_second
        + dot32("tfe,fde->td", d_gate, gate_w)
        + dot32("tfe,fde->td", d_up, up_w)
    )
    d_hidden, gate_low, up_low, packed = lax.optimization_barrier(
        (d_hidden, gate_low, up_low, packed)
    )
    down_total = sum_lines(down_sum, 0)
    gate_sum = sum_spots(gate_low)
    up_sum = sum_spots(up_low)
    gate_total = sum_lines(gate_sum, 2)
    up_total = sum_lines(up_sum, 3)
    d_first, d_gain_one, d_shift_one = norm_back(d_hidden, unit_one, rstd_one, gains[0])
    d_attended = d_first.astype(low_type)
    grad_out = dot32("td,te->de", mixed, d_attended).astype(low_type)
    d_mixed = dot32("te,de->td", d_attended, attention_w[3]).astype(low_type).reshape(head_shape)
    d_probs = dot32("bqhd,bkhd->bhqk", d_mixed, values)
    row_delta = jnp.sum(probs * d_probs, axis=-1, keepdims=True)
    d_scores = (probs * (d_probs - row_delta)).astype(low_type)
    norm_sum = sum_everywhere(jnp.stack([d_gain_one, d_shift_one, d_gain_two, d_shift_two]))
    d_query = dot32("bhqk,bkhd->bqhd", d_scores, key_rows) * scale
    d_keys = dot32("bhqk,bqhd->bkhd", d_scores, queries) * scale
    d_values = dot32("bhqk,bqhd->bkhd", soft_low, d_mixed)
    d_qkv = [
        grad.astype(low_type).reshape(tok_rows, width) for grad in (d_query, d_keys, d_values)
    ]
    grad_values = dot32("td,te->de", inputs, d_qkv[2]).astype(low_type)
    grad_keys = dot32("td,te->de", inputs, d_qkv[1]).astype(low_type)
    grad_query = dot32("td,te->de", inputs, d_qkv[0]).astype(low_type)
    grad_qkv = [grad_query, grad_keys, grad_values]
    d_inputs = d_first
    for k in range(3):
        d_inputs = d_inputs + dot32("te,de->td", d_qkv[k], attention_w[k])
    in_grad = jnp.where(masked, 0.0, d_inputs)

    columns = norm_params.shape[1]
    norm_sum = lax.dynamic_slice_in_dim(norm_sum, my_rows * columns, columns, 1)
    attention_low = sum_copies(grad_qkv + [grad_out])
    mine = sum_lines(sum_spots(attention_low), 1)
    mine, norm_sum = lax.optimization_barrier((mine, norm_sum))
    mine = jnp.where(my_line == 0, down_total, mine)
    mine = jnp.where(my_line == 2, gate_total, mine)
    mine = jnp.where(my_line == 3, up_total, mine).astype(low_type)
    tile_sum = join_copies(mine).reshape(width, width)
    packed = packed.transpose(2, 1, 0, 3, 4).reshape(4, width, width)
    left_low, right_low, moment_one_low, moment_two_low = packed

    step_value = step[0].astype(full_type)
    step_rate = peak_rate * jnp.minimum(
        step_value / warm_steps, (total_steps - step_value) / (total_steps - warm_steps)
    )
    fix_one = 1.0 - jnp.power(beta_one, step_value)
    fix_two = 1.0 - jnp.power(beta_two, step_value)
    turned = dot32("ji,jl->il", left_low, tile_sum)
    high, rest = two_parts(turned)
    rotated = dot32("il,lm->im", high, right_low) + dot32("il,lm->im", rest, right_low)
    mean_one = beta_one * moment_one_low.astype(full_type) + (1.0 - beta_one) * rotated
    mean_two = beta_two * moment_two_low.astype(full_type) + (1.0 - beta_two) * rotated * rotated
    direction = mean_one / fix_one / (jnp.sqrt(mean_two / fix_two) + adam_eps)
    high, rest = two_parts(direction)
    turned = dot32("ij,jl->il", left_low, high) + dot32("ij,jl->il", left_low, rest)
    high, rest = two_parts(turned)
    update = dot32("il,ml->im", high, right_low) + dot32("il,ml->im", rest, right_low)
    results = jnp.stack([rotated, update]).reshape(2, owners, replicas, part, width)
    results = pick(results, my_copy, 2).astype(low_type).transpose(1, 0, 2, 3)
    returned = lax.all_to_all(results, "zero", split_axis=0, concat_axis=0, tiled=True)
    returned = jnp.concatenate([returned[group:tiles], returned[:group]])
    returned = join_copies(returned).transpose(1, 2, 0, 3, 4)
    returned = returned.reshape(tiles, 2, rows, width).astype(full_type)
    turned_rows = returned[:, 0]
    new_first = beta_one * first_moment + (1.0 - beta_one) * turned_rows
    new_second = beta_two * second_moment + (1.0 - beta_two) * turned_rows * turned_rows
    new_master = masters - step_rate * (returned[:, 1] + decay_rate * masters)
    new_norm_first = beta_one * norm_first + (1.0 - beta_one) * norm_sum
    new_norm_second = beta_two * norm_second + (1.0 - beta_two) * norm_sum * norm_sum
    new_norms = norm_params - step_rate * (new_norm_first / fix_one) / (
        jnp.sqrt(new_norm_second / fix_two) + adam_eps
    )
    return (
        layer_out,
        in_grad,
        new_first,
        new_second,
        new_master,
        new_master.astype(low_type),
        new_norm_first,
        new_norm_second,
        new_norms,
    )


def solution(mesh):
    in_specs = (
        P(("dp", "zero"), None),
        P(("dp", "zero"), None),
        P(("dp", "zero"), None),
        P(("dp", "zero"), None),
        P(),
        P(None, "zero", None),
        P(None, "zero"),
        P(None, "zero", None),
        P(None, "zero", None),
        P(None, "zero", None),
        P(None, "zero", None),
        P(None, "zero"),
        P(None, "zero"),
        P(),
    )
    out_specs = (
        P(("dp", "zero"), None),
        P(("dp", "zero"), None),
        P(None, "zero", None),
        P(None, "zero", None),
        P(None, "zero", None),
        P(None, "zero", None),
        P(None, "zero"),
        P(None, "zero"),
        P(None, "zero"),
    )
    return jax.shard_map(shards, mesh=mesh, in_specs=in_specs, out_specs=out_specs, check_vma=False)
```

```python
import math

import jax
import jax.numpy as jnp
import numpy as np
from jax import lax
from jax.sharding import PartitionSpec as P


HEADS = 12

norm_eps = 1e-12
beta_one = 0.9
beta_two = 0.95
adam_eps = 1e-08
peak_rate = 0.1
warm_steps = 5.0
total_steps = 60.0
decay_rate = 0.01
low_type = jnp.bfloat16
full_type = jnp.float32


def alibi_slopes(head_count):

    def power_slopes(power_count):
        first_slope = 2.0 ** (-8.0 / power_count)
        return [first_slope ** (position + 1) for position in range(power_count)]

    nearest = 2 ** int(math.floor(math.log2(head_count)))
    slope_list = power_slopes(nearest)
    slope_list = slope_list + power_slopes(2 * nearest)[0::2][: head_count - nearest]
    return np.array(slope_list, np.float32)


def norm_stats(values):
    row_mean = jnp.mean(values, axis=-1, keepdims=True)
    centered = values - row_mean
    rstd = lax.rsqrt(jnp.mean(centered * centered, axis=-1, keepdims=True) + norm_eps)
    return centered * rstd, rstd


def norm_back(grad, unit, rstd, gain_row):
    scaled = grad * gain_row
    mean_grad = jnp.mean(scaled, axis=-1, keepdims=True)
    mean_prod = jnp.mean(scaled * unit, axis=-1, keepdims=True)
    gain_grad = jnp.sum(grad * unit, axis=0)
    shift_grad = jnp.sum(grad, axis=0)
    return rstd * (scaled - mean_grad - unit * mean_prod), gain_grad, shift_grad


def dot32(spec, left, right):
    return jnp.einsum(spec, left, right, preferred_element_type=full_type)


def two_parts(values):
    high = lax.reduce_precision(values, 8, 7)
    return high.astype(low_type), (values - high).astype(low_type)


def shards(
    tokens,
    out_grad,
    mask_pos,
    repl_id,
    replace_embed,
    masters,
    norm_params,
    first_moment,
    second_moment,
    left_basis,
    right_basis,
    norm_first,
    norm_second,
    step,
):
    seq_count = mask_pos.shape[0]
    tok_rows, width = tokens.shape
    length = tok_rows // seq_count
    heads = HEADS
    head_size = width // heads
    scale = float(head_size) ** (-0.5)
    tiles = masters.shape[0]
    ff = (tiles - 4) // 3
    rows = masters.shape[1]
    replicas = lax.axis_size("dp")
    owners = lax.axis_size("zero")
    my_copy = lax.axis_index("dp")
    my_rows = lax.axis_index("zero")

    part = rows // replicas
    shard_low = masters.astype(low_type)
    sent = lax.dynamic_slice_in_dim(shard_low, my_copy * part, part, 1)
    whole = lax.all_gather(sent, ("zero", "dp"), axis=1, tiled=True)
    norm_whole = lax.all_gather(norm_params.astype(low_type), "zero", axis=1, tiled=True)

    group = ff
    lines = owners // group
    my_line, my_spot = my_rows // group, my_rows % group

    def pick(values, index, axis):
        return lax.dynamic_index_in_dim(values, index, axis, keepdims=False)

    def from_copies(values, shift):
        pairs = [(i, (i + shift) % replicas) for i in range(replicas)]
        return lax.ppermute(values, "dp", pairs)

    def from_spots(values, shift):
        pairs = [(i, i - i % group + (i + shift) % group) for i in range(owners)]
        return lax.ppermute(values, "zero", pairs)

    def from_lines(values, shift):
        pairs = [(i, (i + shift * group) % owners) for i in range(owners)]
        return lax.ppermute(values, "zero", pairs)

    def from_line(values, line, shift):
        pairs = [(i, (i + shift * group) % owners) for i in range(owners) if i // group == line]
        return lax.ppermute(values, "zero", pairs)

    def join_copies(values):
        pieces = [values] + [from_copies(values, shift) for shift in range(1, replicas)]
        if replicas == 2:
            first = my_copy == 0
            return jnp.stack(
                [jnp.where(first, pieces[0], pieces[1]), jnp.where(first, pieces[1], pieces[0])]
            )
        joined = jnp.zeros((replicas,) + values.shape, values.dtype)
        for shift, piece in enumerate(pieces):
            joined = lax.dynamic_update_index_in_dim(
                joined, piece, (my_copy + replicas - shift) % replicas, 0
            )
        return joined

    def sum_everywhere(values):
        total = values
        for shift in range(1, replicas):
            total = total + from_copies(values, shift)
        values = total
        for shift in range(1, group):
            total = total + from_spots(values, shift)
        values = total
        for shift in range(1, lines):
            total = total + from_lines(values, shift)
        return total

    def sum_copies(tile_list):
        parts = [tile.reshape(tile.shape[:-2] + (replicas, -1, width)) for tile in tile_list]
        merge = jnp.stack if parts[0].ndim == 3 else jnp.concatenate

        def part_of(index):
            return merge([pick(tile, index, tile.ndim - 3) for tile in parts])

        total = part_of(my_copy).astype(full_type)
        for shift in range(1, replicas):
            total = total + from_copies(part_of((my_copy + shift) % replicas), shift).astype(full_type)
        return total.astype(low_type)

    def sum_spots(low):
        total = pick(low, my_spot, 0).astype(full_type)
        for shift in range(1, group):
            sent_tile = pick(low, (my_spot + shift) % group, 0)
            moved = from_spots(sent_tile, shift)
            total = total + moved.astype(full_type)
        return total.astype(low_type)

    def sum_lines(low, target):
        total = low.astype(full_type)
        for shift in range(1, lines):
            moved = from_line(low, (target - shift) % lines, shift)
            total = total + moved.astype(full_type)
        return total

    def outgoing(values):
        values = jnp.concatenate([values[tiles - group :], values[: tiles - group]])
        spare = owners - tiles
        return jnp.pad(values, ((0, spare),) + ((0, 0),) * (values.ndim - 1)) if spare else values

    positions = jnp.arange(length, dtype=jnp.int32)
    mask_hits = mask_pos[:, :, None] == positions[None, None, :]
    masked = jnp.any(mask_hits, axis=1).reshape(-1, 1)
    row_ids = jnp.sum(jnp.where(mask_hits, repl_id[:, :, None], 0), axis=1).reshape(-1)
    inputs = jnp.where(masked, jnp.take(replace_embed, row_ids, axis=0), tokens)
    packed = jnp.stack([left_basis, right_basis, first_moment, second_moment], axis=1)
    packed = lax.dynamic_slice_in_dim(packed, my_copy * part, part, 2).astype(low_type)
    whole, inputs, packed = lax.optimization_barrier((whole, inputs, outgoing(packed)))
    packed = lax.all_to_all(packed, "zero", split_axis=0, concat_axis=0, tiled=True)
    gains = norm_whole.astype(full_type)

    slopes = jnp.asarray(alibi_slopes(heads))
    distance = jnp.abs(positions[:, None] - positions[None, :]).astype(full_type)
    alibi_bias = -slopes[:, None, None] * distance[None]
    head_shape = (seq_count, length, heads, head_size)

    qkv = [dot32("td,de->te", inputs, whole[k]).astype(low_type) for k in range(3)]
    queries, key_rows, values = [part_k.reshape(head_shape) for part_k in qkv]
    scores = dot32("bqhd,bkhd->bhqk", queries, key_rows) * scale + alibi_bias[None]
    row_max = jnp.max(scores, axis=-1, keepdims=True)
    log_total = row_max + jnp.log(jnp.sum(jnp.exp(scores - row_max), axis=-1, keepdims=True))
    probs = jnp.exp(scores - log_total)
    soft_low = probs.astype(low_type)
    mixed = dot32("bhqk,bkhd->bqhd", soft_low, values).reshape(tok_rows, width).astype(low_type)
    attended = dot32("td,de->te", mixed, whole[3])
    unit_one, rstd_one = norm_stats(inputs.astype(full_type) + attended)
    hidden = unit_one * gains[0] + gains[1]
    hidden_low = hidden.astype(low_type)

    gate = dot32("td,fde->tfe", hidden_low, whole[4 : 4 + ff])
    up = dot32("td,fde->tfe", hidden_low, whole[4 + ff : 4 + 2 * ff])
    half_erf = 0.5 + 0.5 * lax.erf(gate * math.sqrt(0.5))
    act = gate * half_erf
    slope = half_erf + gate * (jnp.exp(-0.5 * gate * gate) * (1.0 / math.sqrt(2.0 * math.pi)))
    inner_low = (act * up).astype(low_type)
    inner_low, act, up_slope = lax.optimization_barrier((inner_low, act, up * slope))
    branch = dot32("tfe,fed->td", inner_low, whole[4 + 2 * ff :])
    branch, packed = lax.optimization_barrier((branch, packed))
    unit_two, rstd_two = norm_stats(hidden + branch)
    layer_out = (unit_two * gains[2] + gains[3]).astype(low_type)

    d_second, d_gain_two, d_shift_two = norm_back(
        out_grad.astype(full_type), unit_two, rstd_two, gains[2]
    )
    d_branch = d_second.astype(low_type)
    grad_down = [
        dot32("te,td->ed", inner_low[:, f], d_branch).astype(low_type) for f in range(ff)
    ]
    d_branch, grad_down = lax.optimization_barrier((d_branch, grad_down))
    down_low = sum_copies(grad_down)
    packed = join_copies(packed)
    d_inner = dot32("td,fed->tfe", d_branch, whole[4 + 2 * ff :])
    d_gate = (d_inner * up_slope).astype(low_type)
    d_up = (d_inner * act).astype(low_type)
    d_gate, d_up, down_low, packed = lax.optimization_barrier((d_gate, d_up, down_low, packed))
    down_sum = sum_spots(down_low)
    grad_gate = [dot32("td,te->de", hidden_low, d_gate[:, f]).astype(low_type) for f in range(ff)]
    grad_up = [dot32("td,te->de", hidden_low, d_up[:, f]).astype(low_type) for f in range(ff)]
    d_gate, d_up, grad_gate, grad_up = lax.optimization_barrier((d_gate, d_up, grad_gate, grad_up))
    gate_low = sum_copies(grad_gate)
    up_low = sum_copies(grad_up)
    gate_back = dot32("tfe,fde->td", d_gate, whole[4 : 4 + ff])
    d_hidden = d_second + gate_back + dot32("tfe,fde->td", d_up, whole[4 + ff : 4 + 2 * ff])
    d_hidden, gate_low, up_low, down_sum = lax.optimization_barrier(
        (d_hidden, gate_low, up_low, down_sum)
    )
    down_total = sum_lines(down_sum, 0)
    gate_sum = sum_spots(gate_low)
    up_sum = sum_spots(up_low)
    gate_total = sum_lines(gate_sum, 2)
    up_total = sum_lines(up_sum, 3)
    d_first, d_gain_one, d_shift_one = norm_back(d_hidden, unit_one, rstd_one, gains[0])
    d_attended = d_first.astype(low_type)
    grad_out = dot32("td,te->de", mixed, d_attended).astype(low_type)
    d_mixed = dot32("te,de->td", d_attended, whole[3]).astype(low_type).reshape(head_shape)
    d_probs = dot32("bqhd,bkhd->bhqk", d_mixed, values)
    row_delta = jnp.sum(probs * d_probs, axis=-1, keepdims=True)
    d_scores = (probs * (d_probs - row_delta)).astype(low_type)
    norm_sum = sum_everywhere(jnp.stack([d_gain_one, d_shift_one, d_gain_two, d_shift_two]))
    d_query = dot32("bhqk,bkhd->bqhd", d_scores, key_rows) * scale
    d_keys = dot32("bhqk,bqhd->bkhd", d_scores, queries) * scale
    d_values = dot32("bhqk,bqhd->bkhd", soft_low, d_mixed)
    d_qkv = [
        grad.astype(low_type).reshape(tok_rows, width) for grad in (d_query, d_keys, d_values)
    ]
    grad_values = dot32("td,te->de", inputs, d_qkv[2]).astype(low_type)
    grad_keys = dot32("td,te->de", inputs, d_qkv[1]).astype(low_type)
    grad_query = dot32("td,te->de", inputs, d_qkv[0]).astype(low_type)
    grad_qkv = [grad_query, grad_keys, grad_values]
    d_inputs = d_first
    for k in range(3):
        d_inputs = d_inputs + dot32("te,de->td", d_qkv[k], whole[k])
    in_grad = jnp.where(masked, 0.0, d_inputs)

    columns = norm_params.shape[1]
    norm_sum = lax.dynamic_slice_in_dim(norm_sum, my_rows * columns, columns, 1)
    attention_low = sum_copies(grad_qkv + [grad_out])
    mine = sum_lines(sum_spots(attention_low), 1)
    mine, norm_sum, in_grad = lax.optimization_barrier((mine, norm_sum, in_grad))
    mine = jnp.where(my_line == 0, down_total, mine)
    mine = jnp.where(my_line == 2, gate_total, mine)
    mine = jnp.where(my_line == 3, up_total, mine).astype(low_type)
    tile_sum = join_copies(mine).reshape(width, width)
    packed = packed.transpose(2, 1, 0, 3, 4).reshape(4, width, width)
    left_low, right_low, moment_one_low, moment_two_low = packed

    step_value = step[0].astype(full_type)
    step_rate = peak_rate * jnp.minimum(
        step_value / warm_steps, (total_steps - step_value) / (total_steps - warm_steps)
    )
    fix_one = 1.0 - jnp.power(beta_one, step_value)
    fix_two = 1.0 - jnp.power(beta_two, step_value)
    turned = dot32("ji,jl->il", left_low, tile_sum)
    high, rest = two_parts(turned)
    rotated = dot32("il,lm->im", high, right_low) + dot32("il,lm->im", rest, right_low)
    mean_one = beta_one * moment_one_low.astype(full_type) + (1.0 - beta_one) * rotated
    mean_two = beta_two * moment_two_low.astype(full_type) + (1.0 - beta_two) * rotated * rotated
    direction = mean_one / fix_one / (jnp.sqrt(mean_two / fix_two) + adam_eps)
    high, rest = two_parts(direction)
    turned = dot32("ij,jl->il", left_low, high) + dot32("ij,jl->il", left_low, rest)
    high, rest = two_parts(turned)
    update = dot32("il,ml->im", high, right_low) + dot32("il,ml->im", rest, right_low)
    results = jnp.stack([rotated, update]).reshape(2, owners, replicas, part, width)
    results = pick(results, my_copy, 2).astype(low_type).transpose(1, 0, 2, 3)
    returned = lax.all_to_all(results, "zero", split_axis=0, concat_axis=0, tiled=True)
    returned = jnp.concatenate([returned[group:tiles], returned[:group]])
    returned = join_copies(returned).transpose(1, 2, 0, 3, 4)
    returned = returned.reshape(tiles, 2, rows, width).astype(full_type)
    turned_rows = returned[:, 0]
    new_first = beta_one * first_moment + (1.0 - beta_one) * turned_rows
    new_second = beta_two * second_moment + (1.0 - beta_two) * turned_rows * turned_rows
    new_master = masters - step_rate * (returned[:, 1] + decay_rate * masters)
    new_norm_first = beta_one * norm_first + (1.0 - beta_one) * norm_sum
    new_norm_second = beta_two * norm_second + (1.0 - beta_two) * norm_sum * norm_sum
    new_norms = norm_params - step_rate * (new_norm_first / fix_one) / (
        jnp.sqrt(new_norm_second / fix_two) + adam_eps
    )
    return (
        layer_out,
        in_grad,
        new_first,
        new_second,
        new_master,
        new_master.astype(low_type),
        new_norm_first,
        new_norm_second,
        new_norms,
    )


def solution(mesh):
    in_specs = (
        P(("dp", "zero"), None),
        P(("dp", "zero"), None),
        P(("dp", "zero"), None),
        P(("dp", "zero"), None),
        P(),
        P(None, "zero", None),
        P(None, "zero"),
        P(None, "zero", None),
        P(None, "zero", None),
        P(None, "zero", None),
        P(None, "zero", None),
        P(None, "zero"),
        P(None, "zero"),
        P(),
    )
    out_specs = (
        P(("dp", "zero"), None),
        P(("dp", "zero"), None),
        P(None, "zero", None),
        P(None, "zero", None),
        P(None, "zero", None),
        P(None, "zero", None),
        P(None, "zero"),
        P(None, "zero"),
        P(None, "zero"),
    )
    return jax.shard_map(shards, mesh=mesh, in_specs=in_specs, out_specs=out_specs, check_vma=False)
```

```python
import math

import jax
import jax.numpy as jnp
import numpy as np
from jax import lax
from jax.sharding import PartitionSpec as P


HEADS = 12

norm_eps = 1e-12
beta_one = 0.9
beta_two = 0.95
adam_eps = 1e-08
peak_rate = 0.1
warm_steps = 5.0
total_steps = 60.0
decay_rate = 0.01
low_type = jnp.bfloat16
full_type = jnp.float32


def alibi_slopes(head_count):

    def power_slopes(power_count):
        first_slope = 2.0 ** (-8.0 / power_count)
        return [first_slope ** (position + 1) for position in range(power_count)]

    nearest = 2 ** int(math.floor(math.log2(head_count)))
    slope_list = power_slopes(nearest)
    slope_list = slope_list + power_slopes(2 * nearest)[0::2][: head_count - nearest]
    return np.array(slope_list, np.float32)


def norm_stats(values):
    row_mean = jnp.mean(values, axis=-1, keepdims=True)
    centered = values - row_mean
    rstd = lax.rsqrt(jnp.mean(centered * centered, axis=-1, keepdims=True) + norm_eps)
    return centered * rstd, rstd


def norm_back(grad, unit, rstd, gain_row):
    scaled = grad * gain_row
    mean_grad = jnp.mean(scaled, axis=-1, keepdims=True)
    mean_prod = jnp.mean(scaled * unit, axis=-1, keepdims=True)
    gain_grad = jnp.sum(grad * unit, axis=0)
    shift_grad = jnp.sum(grad, axis=0)
    return rstd * (scaled - mean_grad - unit * mean_prod), gain_grad, shift_grad


def dot32(spec, left, right):
    return jnp.einsum(spec, left, right, preferred_element_type=full_type)


def shards(
    tokens,
    out_grad,
    mask_pos,
    repl_id,
    replace_embed,
    masters,
    norm_params,
    first_moment,
    second_moment,
    left_basis,
    right_basis,
    norm_first,
    norm_second,
    step,
):
    seq_count = mask_pos.shape[0]
    tok_rows, width = tokens.shape
    length = tok_rows // seq_count
    heads = HEADS
    head_size = width // heads
    scale = float(head_size) ** (-0.5)
    tiles = masters.shape[0]
    ff = (tiles - 4) // 3
    rows = masters.shape[1]
    replicas = lax.axis_size("dp")
    owners = lax.axis_size("zero")
    my_copy = lax.axis_index("dp")
    my_rows = lax.axis_index("zero")

    part = rows // replicas
    shard_low = masters.astype(low_type)
    sent = lax.dynamic_slice_in_dim(shard_low, my_copy * part, part, 1)
    whole = lax.all_gather(sent, ("zero", "dp"), axis=1, tiled=True)
    norm_whole = lax.all_gather(norm_params.astype(low_type), "zero", axis=1, tiled=True)

    group = ff
    lines = owners // group
    my_line, my_spot = my_rows // group, my_rows % group

    def pick(values, index, axis):
        return lax.dynamic_index_in_dim(values, index, axis, keepdims=False)

    def from_copies(values, shift):
        pairs = [(i, (i + shift) % replicas) for i in range(replicas)]
        return lax.ppermute(values, "dp", pairs)

    def from_spots(values, shift):
        pairs = [(i, i - i % group + (i + shift) % group) for i in range(owners)]
        return lax.ppermute(values, "zero", pairs)

    def from_lines(values, shift):
        pairs = [(i, (i + shift * group) % owners) for i in range(owners)]
        return lax.ppermute(values, "zero", pairs)

    def from_line(values, line, shift):
        pairs = [(i, (i + shift * group) % owners) for i in range(owners) if i // group == line]
        return lax.ppermute(values, "zero", pairs)

    def join_copies(values):
        pieces = [values] + [from_copies(values, shift) for shift in range(1, replicas)]
        if replicas == 2:
            first = my_copy == 0
            return jnp.stack(
                [jnp.where(first, pieces[0], pieces[1]), jnp.where(first, pieces[1], pieces[0])]
            )
        joined = jnp.zeros((replicas,) + values.shape, values.dtype)
        for shift, piece in enumerate(pieces):
            joined = lax.dynamic_update_index_in_dim(
                joined, piece, (my_copy + replicas - shift) % replicas, 0
            )
        return joined

    def sum_everywhere(values):
        total = values
        for shift in range(1, replicas):
            total = total + from_copies(values, shift)
        values = total
        for shift in range(1, group):
            total = total + from_spots(values, shift)
        values = total
        for shift in range(1, lines):
            total = total + from_lines(values, shift)
        return total

    def sum_copies(tile_list):
        parts = [tile.reshape(tile.shape[:-2] + (replicas, -1, width)) for tile in tile_list]
        merge = jnp.stack if parts[0].ndim == 3 else jnp.concatenate

        def part_of(index):
            return merge([pick(tile, index, tile.ndim - 3) for tile in parts])

        total = part_of(my_copy).astype(full_type)
        for shift in range(1, replicas):
            total = total + from_copies(part_of((my_copy + shift) % replicas), shift).astype(full_type)
        return total.astype(low_type)

    def sum_spots(low):
        total = pick(low, my_spot, 0).astype(full_type)
        for shift in range(1, group):
            sent_tile = pick(low, (my_spot + shift) % group, 0)
            moved = from_spots(sent_tile, shift)
            total = total + moved.astype(full_type)
        return total.astype(low_type)

    def sum_lines(low, target):
        total = low.astype(full_type)
        for shift in range(1, lines):
            moved = from_line(low, (target - shift) % lines, shift)
            total = total + moved.astype(full_type)
        return total

    def outgoing(values):
        values = jnp.concatenate([values[tiles - group :], values[: tiles - group]])
        spare = owners - tiles
        return jnp.pad(values, ((0, spare),) + ((0, 0),) * (values.ndim - 1)) if spare else values

    positions = jnp.arange(length, dtype=jnp.int32)
    mask_hits = mask_pos[:, :, None] == positions[None, None, :]
    masked = jnp.any(mask_hits, axis=1).reshape(-1, 1)
    row_ids = jnp.sum(jnp.where(mask_hits, repl_id[:, :, None], 0), axis=1).reshape(-1)
    inputs = jnp.where(masked, jnp.take(replace_embed, row_ids, axis=0), tokens)
    packed = jnp.stack([left_basis, right_basis, first_moment, second_moment], axis=1)
    packed = lax.dynamic_slice_in_dim(packed, my_copy * part, part, 2).astype(low_type)
    whole, inputs, packed = lax.optimization_barrier((whole, inputs, outgoing(packed)))
    packed = lax.all_to_all(packed, "zero", split_axis=0, concat_axis=0, tiled=True)
    gains = norm_whole.astype(full_type)

    slopes = jnp.asarray(alibi_slopes(heads))
    distance = jnp.abs(positions[:, None] - positions[None, :]).astype(full_type)
    alibi_bias = -slopes[:, None, None] * distance[None]
    head_shape = (seq_count, length, heads, head_size)

    qkv = [dot32("td,de->te", inputs, whole[k]).astype(low_type) for k in range(3)]
    queries, key_rows, values = [part_k.reshape(head_shape) for part_k in qkv]
    scores = dot32("bqhd,bkhd->bhqk", queries, key_rows) * scale + alibi_bias[None]
    row_max = jnp.max(scores, axis=-1, keepdims=True)
    log_total = row_max + jnp.log(jnp.sum(jnp.exp(scores - row_max), axis=-1, keepdims=True))
    probs = jnp.exp(scores - log_total)
    soft_low = probs.astype(low_type)
    mixed = dot32("bhqk,bkhd->bqhd", soft_low, values).reshape(tok_rows, width).astype(low_type)
    attended = dot32("td,de->te", mixed, whole[3])
    unit_one, rstd_one = norm_stats(inputs.astype(full_type) + attended)
    hidden = unit_one * gains[0] + gains[1]
    hidden_low = hidden.astype(low_type)

    gate = dot32("td,fde->tfe", hidden_low, whole[4 : 4 + ff])
    up = dot32("td,fde->tfe", hidden_low, whole[4 + ff : 4 + 2 * ff])
    half_erf = 0.5 + 0.5 * lax.erf(gate * math.sqrt(0.5))
    act = gate * half_erf
    slope = half_erf + gate * (jnp.exp(-0.5 * gate * gate) * (1.0 / math.sqrt(2.0 * math.pi)))
    inner_low = (act * up).astype(low_type)
    inner_low, act, up_slope = lax.optimization_barrier((inner_low, act, up * slope))
    branch = dot32("tfe,fed->td", inner_low, whole[4 + 2 * ff :])
    branch, packed = lax.optimization_barrier((branch, packed))
    unit_two, rstd_two = norm_stats(hidden + branch)
    layer_out = (unit_two * gains[2] + gains[3]).astype(low_type)

    d_second, d_gain_two, d_shift_two = norm_back(
        out_grad.astype(full_type), unit_two, rstd_two, gains[2]
    )
    d_branch = d_second.astype(low_type)
    grad_down = [
        dot32("te,td->ed", inner_low[:, f], d_branch).astype(low_type) for f in range(ff)
    ]
    d_branch, grad_down = lax.optimization_barrier((d_branch, grad_down))
    down_low = sum_copies(grad_down)
    packed = join_copies(packed)
    d_inner = dot32("td,fed->tfe", d_branch, whole[4 + 2 * ff :])
    d_gate = (d_inner * up_slope).astype(low_type)
    d_up = (d_inner * act).astype(low_type)
    d_gate, d_up, down_low, packed = lax.optimization_barrier((d_gate, d_up, down_low, packed))
    down_sum = sum_spots(down_low)
    grad_gate = [dot32("td,te->de", hidden_low, d_gate[:, f]).astype(low_type) for f in range(ff)]
    grad_up = [dot32("td,te->de", hidden_low, d_up[:, f]).astype(low_type) for f in range(ff)]
    d_gate, d_up, grad_gate, grad_up = lax.optimization_barrier((d_gate, d_up, grad_gate, grad_up))
    gate_low = sum_copies(grad_gate)
    up_low = sum_copies(grad_up)
    gate_back = dot32("tfe,fde->td", d_gate, whole[4 : 4 + ff])
    d_hidden = d_second + gate_back + dot32("tfe,fde->td", d_up, whole[4 + ff : 4 + 2 * ff])
    d_hidden, gate_low, up_low, down_sum = lax.optimization_barrier(
        (d_hidden, gate_low, up_low, down_sum)
    )
    down_total = sum_lines(down_sum, 0)
    gate_sum = sum_spots(gate_low)
    up_sum = sum_spots(up_low)
    gate_total = sum_lines(gate_sum, 2)
    up_total = sum_lines(up_sum, 3)
    d_first, d_gain_one, d_shift_one = norm_back(d_hidden, unit_one, rstd_one, gains[0])
    d_attended = d_first.astype(low_type)
    grad_out = dot32("td,te->de", mixed, d_attended).astype(low_type)
    d_mixed = dot32("te,de->td", d_attended, whole[3]).astype(low_type).reshape(head_shape)
    d_probs = dot32("bqhd,bkhd->bhqk", d_mixed, values)
    row_delta = jnp.sum(probs * d_probs, axis=-1, keepdims=True)
    d_scores = (probs * (d_probs - row_delta)).astype(low_type)
    norm_sum = sum_everywhere(jnp.stack([d_gain_one, d_shift_one, d_gain_two, d_shift_two]))
    d_query = dot32("bhqk,bkhd->bqhd", d_scores, key_rows) * scale
    d_keys = dot32("bhqk,bqhd->bkhd", d_scores, queries) * scale
    d_values = dot32("bhqk,bqhd->bkhd", soft_low, d_mixed)
    d_qkv = [
        grad.astype(low_type).reshape(tok_rows, width) for grad in (d_query, d_keys, d_values)
    ]
    grad_values = dot32("td,te->de", inputs, d_qkv[2]).astype(low_type)
    grad_keys = dot32("td,te->de", inputs, d_qkv[1]).astype(low_type)
    grad_query = dot32("td,te->de", inputs, d_qkv[0]).astype(low_type)
    grad_qkv = [grad_query, grad_keys, grad_values]
    d_inputs = d_first
    for k in range(3):
        d_inputs = d_inputs + dot32("te,de->td", d_qkv[k], whole[k])
    in_grad = jnp.where(masked, 0.0, d_inputs)

    columns = norm_params.shape[1]
    norm_sum = lax.dynamic_slice_in_dim(norm_sum, my_rows * columns, columns, 1)
    attention_low = sum_copies(grad_qkv + [grad_out])
    mine = sum_lines(sum_spots(attention_low), 1)
    mine, norm_sum, in_grad = lax.optimization_barrier((mine, norm_sum, in_grad))
    mine = jnp.where(my_line == 0, down_total, mine)
    mine = jnp.where(my_line == 2, gate_total, mine)
    mine = jnp.where(my_line == 3, up_total, mine).astype(low_type)
    tile_sum = join_copies(mine).reshape(width, width)
    packed = packed.transpose(2, 1, 0, 3, 4).reshape(4, width, width)
    left_low, right_low, moment_one_low, moment_two_low = packed

    step_value = step[0].astype(full_type)
    step_rate = peak_rate * jnp.minimum(
        step_value / warm_steps, (total_steps - step_value) / (total_steps - warm_steps)
    )
    fix_one = 1.0 - jnp.power(beta_one, step_value)
    fix_two = 1.0 - jnp.power(beta_two, step_value)
    turned = dot32("ji,jl->il", left_low, tile_sum)
    rotated = dot32("il,lm->im", turned.astype(low_type), right_low)
    mean_one = beta_one * moment_one_low.astype(full_type) + (1.0 - beta_one) * rotated
    mean_two = beta_two * moment_two_low.astype(full_type) + (1.0 - beta_two) * rotated * rotated
    direction = mean_one / fix_one / (jnp.sqrt(mean_two / fix_two) + adam_eps)
    turned = dot32("ij,jl->il", left_low, direction.astype(low_type))
    update = dot32("il,ml->im", turned.astype(low_type), right_low)
    results = jnp.stack([rotated, update]).reshape(2, owners, replicas, part, width)
    results = pick(results, my_copy, 2).astype(low_type).transpose(1, 0, 2, 3)
    returned = lax.all_to_all(results, "zero", split_axis=0, concat_axis=0, tiled=True)
    returned = jnp.concatenate([returned[group:tiles], returned[:group]])
    returned = join_copies(returned).transpose(1, 2, 0, 3, 4)
    returned = returned.reshape(tiles, 2, rows, width).astype(full_type)
    turned_rows = returned[:, 0]
    new_first = beta_one * first_moment + (1.0 - beta_one) * turned_rows
    new_second = beta_two * second_moment + (1.0 - beta_two) * turned_rows * turned_rows
    new_master = masters - step_rate * (returned[:, 1] + decay_rate * masters)
    new_norm_first = beta_one * norm_first + (1.0 - beta_one) * norm_sum
    new_norm_second = beta_two * norm_second + (1.0 - beta_two) * norm_sum * norm_sum
    new_norms = norm_params - step_rate * (new_norm_first / fix_one) / (
        jnp.sqrt(new_norm_second / fix_two) + adam_eps
    )
    return (
        layer_out,
        in_grad,
        new_first,
        new_second,
        new_master,
        new_master.astype(low_type),
        new_norm_first,
        new_norm_second,
        new_norms,
    )


def solution(mesh):
    in_specs = (
        P(("dp", "zero"), None),
        P(("dp", "zero"), None),
        P(("dp", "zero"), None),
        P(("dp", "zero"), None),
        P(),
        P(None, "zero", None),
        P(None, "zero"),
        P(None, "zero", None),
        P(None, "zero", None),
        P(None, "zero", None),
        P(None, "zero", None),
        P(None, "zero"),
        P(None, "zero"),
        P(),
    )
    out_specs = (
        P(("dp", "zero"), None),
        P(("dp", "zero"), None),
        P(None, "zero", None),
        P(None, "zero", None),
        P(None, "zero", None),
        P(None, "zero", None),
        P(None, "zero"),
        P(None, "zero"),
        P(None, "zero"),
    )
    return jax.shard_map(shards, mesh=mesh, in_specs=in_specs, out_specs=out_specs, check_vma=False)
```
